16 devices in a mesh: rep: 2 (over y, z), dp: 8 (over x, core).
Axes of the slice: x: 4, y: 2, z: 1, core: 2. Of those that a mesh axis runs over, the one named last changes fastest.
The devices are a block of a 4x4x8 slice.
Arguments:
- x: bfloat16 [16, 2048, 1024], P(('rep', 'dp')), parts along dimension 0
- dy: bfloat16 [16, 2048, 1024], P(('rep', 'dp')), parts along dimension 0
- w_gate: bfloat16 [2, 1024, 2560], P(None, 'dp')
- w_up: bfloat16 [2, 1024, 2560], P(None, 'dp')
- w_down: bfloat16 [2, 2560, 1024], P(None, 'dp')
- m_w_gate: float32 [2, 1024, 2560], P(None, 'dp')
- m_w_up: float32 [2, 1024, 2560], P(None, 'dp')
- m_w_down: float32 [2, 2560, 1024], P(None, 'dp')
- v_w_gate: float32 [2, 1024, 2560], P(None, 'dp')
- v_w_up: float32 [2, 1024, 2560], P(None, 'dp')
- v_w_down: float32 [2, 2560, 1024], P(None, 'dp')
Outputs:
- output 1: bfloat16 [4, 1024, 2560], P('rep', 'dp'), parts along dimension 0
- output 2: bfloat16 [4, 1024, 2560], P('rep', 'dp'), parts along dimension 0
- output 3: bfloat16 [4, 2560, 1024], P('rep', 'dp'), parts along dimension 0
- output 4: float32 [4, 1024, 2560], P('rep', 'dp'), parts along dimension 0
- output 5: float32 [4, 1024, 2560], P('rep', 'dp'), parts along dimension 0
- output 6: float32 [4, 2560, 1024], P('rep', 'dp'), parts along dimension 0
- output 7: float32 [4, 1024, 2560], P('rep', 'dp'), parts along dimension 0
- output 8: float32 [4, 1024, 2560], P('rep', 'dp'), parts along dimension 0
- output 9: float32 [4, 2560, 1024], P('rep', 'dp'), parts along dimension 0
There are 2 independent parts. The reference program is written for one: setup_inputs(seed, part) draws one part's arguments, and reference() takes and returns one part's arrays. A program takes and returns all parts, laid end to end along the dimension named above; an argument that names none is the same for every part.
All inputs are finite; a program needn't handle non-finite values.
Results may differ from the reference program's by a relative error of at most 0.022.
Values are sent between devices in bfloat16 or wider.
A program may use at most 768 MiB of HBM per device.

```python
import jax
import jax.numpy as jnp
from jax import lax

SEQUENCES = 8
TOKENS = 2048
D = 1024
FF = 2560
LAYERS = 2
NAMES = ("w_gate", "w_up", "w_down")
SHAPES = {"w_gate": (LAYERS, D, FF), "w_up": (LAYERS, D, FF), "w_down": (LAYERS, FF, D)}


def bump(key, n, height):
    away = (jnp.arange(n, dtype=jnp.int32) - jax.random.randint(key, (), 0, n, jnp.int32)) % n
    return jnp.where(away < n // 8, height, 1.0)


def together(key, own, strength):
    shared = jax.random.normal(key, own.shape[1:], jnp.float32)
    return (own + strength * shared) * lax.rsqrt(1 + strength * strength)


def setup_inputs(seed: int = 0, part: int = 0) -> dict:
    kx, kdy, ka, kb, kz, kf, kh, kl, *keys = jax.random.split(jax.random.key(seed), 8 + 3 * len(NAMES))
    kx, kdy, ka, kb = (jax.random.fold_in(k, part) for k in (kx, kdy, ka, kb))
    kw, km, kv = (keys[i::3] for i in range(3))
    shape = (SEQUENCES, TOKENS, D)
    much_x, much_dy = jax.random.uniform(kz, (2,), jnp.float32, 0.0, 1.0)
    loud = 2.0 ** jax.random.uniform(jax.random.fold_in(kz, 1), (), jnp.float32, -1.0, 2.0)
    layers = 2.0 ** jax.random.uniform(kl, (LAYERS, 1, 1), jnp.float32, -1.0, 1.0)
    x = together(ka, jax.random.normal(kx, shape, jnp.float32), much_x) * bump(kf, D, 4.0)
    dy = together(kb, jax.random.normal(kdy, shape, jnp.float32), much_dy)
    drawn = {"x": x.astype(jnp.bfloat16), "dy": (loud * dy * (SEQUENCES * TOKENS) ** -0.5).astype(jnp.bfloat16)}
    for key, name in zip(kw, NAMES, strict=True):
        w = jax.random.normal(key, SHAPES[name], jnp.float32) * SHAPES[name][1] ** -0.5
        drawn[name] = (w * {"w_gate": 1.0, "w_up": bump(kh, FF, 4.0), "w_down": layers}[name]).astype(jnp.bfloat16)
    for key, name in zip(km, NAMES, strict=True):
        drawn[f"m_{name}"] = 0.1 * jax.random.normal(key, SHAPES[name], jnp.float32)
    for key, name in zip(kv, NAMES, strict=True):
        drawn[f"v_{name}"] = jax.random.uniform(key, SHAPES[name], jnp.float32, 0.005, 0.015)
    return drawn


def matmul(a, w):
    return jnp.dot(a, w, preferred_element_type=jnp.float32).astype(jnp.bfloat16)


def normed(h):
    wide = h.astype(jnp.float32)
    scale = lax.rsqrt(jnp.mean(wide**2, -1, keepdims=True) + 1e-6)
    return (wide * scale).astype(jnp.bfloat16)


def layer(h, w):
    a = normed(h)
    gate = jnp.dot(a, w["w_gate"], preferred_element_type=jnp.float32)
    up = jnp.dot(a, w["w_up"], preferred_element_type=jnp.float32)
    return h + matmul((jax.nn.silu(gate) * up).astype(jnp.bfloat16), w["w_down"])


def adamw(w, m, v, g):
    m = 0.9 * m + 0.1 * g
    v = 0.95 * v + 0.05 * g * g
    step = m * lax.rsqrt(v + 1e-8) + 0.1 * w
    return (w - 0.02 * step).astype(jnp.bfloat16), m, v


def clipped(gradients, sum_of_squares, count):
    factor = jnp.minimum(1.0, 0.5 * lax.rsqrt(sum_of_squares / count + 1e-30))
    return [g * factor for g in gradients]


def stack(weights, h):
    return lax.scan(lambda h, w: (layer(h, w), None), h, weights)[0]


def reference(x, dy, w_gate, w_up, w_down, m_w_gate, m_w_up, m_w_down, v_w_gate, v_w_up, v_w_down):
    weights = dict(zip(NAMES, (w_gate, w_up, w_down), strict=True))

    def take(so_far, sequence):
        h, by_y = sequence
        _, back = jax.vjp(lambda w: stack(w, h), weights)
        return jax.tree.map(lambda total, term: total + term.astype(jnp.float32), so_far, back(by_y)[0]), None

    none_yet = {name: jnp.zeros(w.shape, jnp.float32) for name, w in weights.items()}
    by_weights, _ = lax.scan(take, none_yet, (x, dy))
    gradients = [by_weights[name].astype(jnp.bfloat16).astype(jnp.float32) for name in NAMES]
    gradients = clipped(gradients, sum(jnp.sum(g * g) for g in gradients), sum(g.size for g in gradients))
    new = [
        adamw(w.astype(jnp.float32), m, v, g)
        for w, m, v, g in zip((w_gate, w_up, w_down), (m_w_gate, m_w_up, m_w_down), (v_w_gate, v_w_up, v_w_down), gradients, strict=True)
    ]
    return tuple(one[which] for which in range(3) for one in new)
```

```python
import functools

import jax
import jax.numpy as jnp
from jax import lax
from jax.experimental import pallas as pl
from jax.experimental.pallas import tpu as pltpu
from jax.sharding import PartitionSpec as P

MESH = pl.DeviceIdType.MESH
ANY = pl.BlockSpec(memory_space=pl.ANY)
F32, BF16 = jnp.float32, jnp.bfloat16
LANES = 128
NT = (((1,), (1,)), ((), ()))
TN = (((0,), (0,)), ((), ()))


def places(n):
    me = lax.axis_index("dp")
    core, chips = lax.rem(me, 2), n // 2
    chip = me // 2
    around = lambda k: lax.rem(chip + k, chips) * 2 + core
    return me, chip, core, me + 1 - 2 * core, around(1), around(chips - 1), around(2)


def greet(*others):
    barrier = pltpu.get_barrier_semaphore()
    for other in others:
        pl.semaphore_signal(barrier, inc=1, device_id={"dp": other}, device_id_type=MESH)
    pl.semaphore_wait(barrier, len(others))


def norm_rows(wide):
    scale = lax.rsqrt(jnp.mean(wide * wide, -1, keepdims=True) + 1e-6)
    return (wide * scale).astype(BF16)


def forward_kernel(n, x_ref, wg_ref, wu_ref, wd_ref, g_ref, u_ref, d_ref, a_out, h_out, gate_out, up_out,
                   own_g, own_u, own_d, h, a, hidden, wchunk, wdown, stage,
                   send, recv, own_sem, out_sem, w_sem, stage_sem, misc):
    me, chip, core, partner, right, left, far = places(n)
    layers = wg_ref.shape[0]
    tokens, d = x_ref.shape
    chunks, _, width = gate_out.shape[1:]
    chips = n // 2
    tile = stage.shape[2]
    tiles = tokens // tile
    span = g_ref.shape[2] // chips

    order = [(l, w, o) for l in range(layers) for w, o in ((g_ref, own_g), (u_ref, own_u), (d_ref, own_d))]

    loads = [pltpu.make_async_copy(src.at[l], o.at[l], own_sem.at[3 * l + i])
             for l in range(layers) for i, (src, o) in enumerate(((wg_ref, own_g), (wu_ref, own_u), (wd_ref, own_d)))]
    for one in loads:
        one.start()
    load_x = pltpu.make_async_copy(x_ref, h, misc.at[0])
    load_x.start()
    greet(partner, right, left)

    def rows(m, device, part=None):
        l, w, o = order[m]
        count = o.shape[1]
        if part is None:
            return w.at[l, pl.ds(device * count, count)]
        return w.at[l, pl.ds(device * count + part * (count // 2), count // 2)]

    def ag(m, kind):
        l, w, o = order[m]
        src, to = [
            (None, right), (None, left),
            (rows(m, left, 0), right), (rows(m, right, 1), left),
            (None, partner), (rows(m, left), partner), (rows(m, right), partner),
            (rows(m, far, 0), partner), (rows(m, far, 1), partner),
        ][kind]
        dst = rows(m, me) if src is None else src
        return pltpu.make_async_remote_copy(o.at[l] if src is None else src, dst, send.at[m, kind], recv.at[m, kind],
                                            device_id={"dp": to}, device_id_type=MESH)

    kept = []

    def begin(m):
        loads[m].wait()
        ag(m, 0).start()
        ag(m, 1).start()
        ag(m, 4).start()
        l, w, o = order[m]
        copy = pltpu.make_async_copy(o.at[l], rows(m, me), out_sem.at[m])
        copy.start()
        kept.append(copy)

    def pass_on(m):
        ag(m, 0).wait_recv()
        ag(m, 2).start()
        ag(m, 5).start()
        ag(m, 1).wait_recv()
        ag(m, 3).start()
        ag(m, 6).start()

    def hand_over(m):
        ag(m, 2).wait_recv()
        ag(m, 7).start()
        ag(m, 3).wait_recv()
        ag(m, 8).start()

    def complete(m):
        for kind in (4, 5, 6, 7, 8):
            ag(m, kind).wait_recv()
        kept[m].wait()

    begin(0)
    begin(1)
    load_x.wait()

    def norm_step(t, _):
        r = pl.ds(pl.multiple_of(t * 256, 256), 256)
        a[r, :] = norm_rows(h[r, :].astype(F32))
        return 0
    lax.fori_loop(0, tokens // 256, norm_step, 0)
    a_copy = pltpu.make_async_copy(a, a_out.at[0], misc.at[1])
    a_copy.start()

    def w_loads(l, j, slot):
        return [pltpu.make_async_copy(w.at[l, :, pl.ds(c * span + j * LANES, LANES)], wchunk.at[slot, i, :, pl.ds(c * LANES, LANES)],
                                      w_sem.at[slot, i, c])
                for i, w in enumerate((g_ref, u_ref)) for c in range(chips)]

    def gate_up(l, between, with_hidden):
        for one in w_loads(l, 0, 0):
            one.start()
        for j in range(chunks):
            slot = j % 2
            for one in w_loads(l, j, slot):
                one.wait()
            if j + 1 < chunks:
                for one in w_loads(l, j + 1, 1 - slot):
                    one.start()

            def step(t, _):
                half = lax.rem(t, 2)
                r = pl.ds(pl.multiple_of(t * tile, tile), tile)

                def outs(t_):
                    rr = pl.ds(pl.multiple_of(t_ * tile, tile), tile)
                    hh = lax.rem(t_, 2)
                    return [pltpu.make_async_copy(stage.at[hh, i], o.at[l, j, rr], stage_sem.at[hh, i])
                            for i, o in enumerate((gate_out, up_out))]

                @pl.when(t >= (2 if j == 0 else 0))
                def _():
                    for one in outs(t):
                        one.wait()
                rows_a = a[r, :]
                stage[half, 0] = jnp.dot(rows_a, wchunk[slot, 0], preferred_element_type=F32)
                stage[half, 1] = jnp.dot(rows_a, wchunk[slot, 1], preferred_element_type=F32)
                if with_hidden:
                    gate, up = stage[half, 0], stage[half, 1]
                    hidden[r, pl.ds(j * width, width)] = (jax.nn.silu(gate) * up).astype(BF16)
                for one in outs(t):
                    one.start()
                return 0
            lax.fori_loop(0, tiles, step, 0)
            between(j)
        for half in range(2):
            for i, o in enumerate((gate_out, up_out)):
                pltpu.make_async_copy(stage.at[half, i], o.at[l, 0, pl.ds(0, tile)], stage_sem.at[half, i]).wait()

    pass_on(0)
    pass_on(1)
    begin(2)
    begin(3)
    hand_over(0)
    hand_over(1)
    complete(0)
    complete(1)

    def first(j):
        if j == 2:
            pass_on(2)
            begin(4)
        if j == 4:
            pass_on(3)
    gate_up(0, first, True)

    hand_over(2)
    complete(2)
    down = [pltpu.make_async_copy(d_ref.at[0, pl.ds(c * span + j * LANES, LANES)], wdown.at[pl.ds(j * width + c * LANES, LANES)], misc.at[3 + j * chips + c])
            for j in range(chunks) for c in range(chips)]
    for one in down:
        one.start()
    a_copy.wait()
    for one in down:
        one.wait()

    def down_step(t, _):
        r = pl.ds(pl.multiple_of(t * tile, tile), tile)
        y = jnp.dot(hidden[r, :], wdown[...], preferred_element_type=F32).astype(BF16)
        h1 = (h[r, :].astype(F32) + y.astype(F32)).astype(BF16)
        h[r, :] = h1
        a[r, :] = norm_rows(h1.astype(F32))
        return 0
    lax.fori_loop(0, tiles, down_step, 0)
    h_copy = pltpu.make_async_copy(h, h_out, misc.at[2])
    h_copy.start()
    a_copy = pltpu.make_async_copy(a, a_out.at[1], misc.at[1])
    a_copy.start()
    pass_on(4)
    begin(5)
    hand_over(3)
    hand_over(4)
    complete(3)
    complete(4)

    def second(j):
        if j == 2:
            pass_on(5)
    gate_up(1, second, False)
    hand_over(5)
    complete(5)
    h_copy.wait()
    a_copy.wait()
    for m in range(len(order)):
        for kind in range(9):
            ag(m, kind).wait_send()


def forward(n, x, wg, wu, wd):
    tokens, d = x.shape
    layers, _, ff = wg.shape
    chips = n // 2
    width = chips * LANES
    chunks = ff // width
    tile = 512
    sds = jax.ShapeDtypeStruct
    dma = pltpu.SemaphoreType.DMA
    return pl.pallas_call(
        functools.partial(forward_kernel, n),
        name="forward",
        out_shape=(
            sds((layers, d, ff), BF16), sds((layers, d, ff), BF16), sds((layers, ff, d), BF16),
            sds((layers, tokens, d), BF16), sds((tokens, d), BF16),
            sds((layers, chunks, tokens, width), F32), sds((layers, chunks, tokens, width), F32),
        ),
        in_specs=[ANY] * 4,
        out_specs=(ANY,) * 7,
        scratch_shapes=[
            pltpu.VMEM(wg.shape, BF16), pltpu.VMEM(wu.shape, BF16), pltpu.VMEM(wd.shape, BF16),
            pltpu.VMEM((tokens, d), BF16), pltpu.VMEM((tokens, d), BF16), pltpu.VMEM((tokens, ff), BF16),
            pltpu.VMEM((2, 2, d, width), BF16), pltpu.VMEM((ff, d), BF16), pltpu.VMEM((2, 2, tile, width), F32),
            dma((3 * layers, 9)), dma((3 * layers, 9)), dma((3 * layers,)), dma((3 * layers,)),
            dma((2, 2, chips)), dma((2, 2)), dma((3 + chunks * chips,)),
        ],
        compiler_params=pltpu.CompilerParams(collective_id=0, has_side_effects=True, vmem_limit_bytes=60 * 1024 * 1024),
    )(x, wg, wu, wd)


SLOTS = 4


def backward_kernel(n, dy_ref, g_ref, u_ref, d_ref, a_ref, h_ref, gate_ref, up_ref, gg_out, gu_out, gd_out, sq_out,
                    ct, at, nat, da, hid, hid_t, dg, du, dh, stage, wd, wgu, own, out_p, in_p, out_1, in_1, out_2, in_2, fin,
                    gg, gu, gd, sq, squares,
                    stage_sem, wd_sem, wgu_sem, p_send, p_recv, s1_send, s1_recv, s2_send, s2_recv, f_send, f_recv, q_send, q_recv, misc):
    me, chip, core, partner, right, left, far = places(n)
    layers, chunks, tokens, width = gate_ref.shape
    d = dy_ref.shape[1]
    chips = n // 2
    span = g_ref.shape[2] // chips
    share = gd.shape[1]
    tile = stage.shape[2]
    tiles = tokens // tile
    sub = 256
    total = layers * chunks
    half = d // 2

    def layer_of(jj):
        return layers - 1 - jj // chunks

    def stage_loads(s):
        jj, t = s // tiles, lax.rem(s, tiles)
        slot = lax.rem(s, 2)
        r = pl.ds(pl.multiple_of(t * tile, tile), tile)
        return [pltpu.make_async_copy(ref.at[layer_of(jj), lax.rem(jj, chunks), r], stage.at[slot, i], stage_sem.at[slot, i])
                for i, ref in enumerate((gate_ref, up_ref))]

    def wd_loads(jj):
        l, j, slot = layer_of(jj), lax.rem(jj, chunks), lax.rem(jj, 2)
        return [pltpu.make_async_copy(d_ref.at[l, pl.ds(pl.multiple_of(c * span + j * LANES, LANES), LANES)],
                                      wd.at[slot, pl.ds(c * LANES, LANES)], wd_sem.at[slot, c]) for c in range(chips)]

    def wgu_loads(jj):
        l, j, slot = layer_of(jj), lax.rem(jj, chunks), lax.rem(jj, 2)
        return [pltpu.make_async_copy(ref.at[l, :, pl.ds(pl.multiple_of(c * span + j * LANES, LANES), LANES)],
                                      wgu.at[slot, i, :, pl.ds(c * LANES, LANES)], wgu_sem.at[slot, i, c])
                for i, ref in enumerate((g_ref, u_ref)) for c in range(chips)]

    first = [pltpu.make_async_copy(a_ref.at[layers - 1], nat, misc.at[0]), pltpu.make_async_copy(dy_ref, ct, misc.at[1])]
    for one in first + stage_loads(0) + wd_loads(0) + wgu_loads(0):
        one.start()

    barrier = pltpu.get_barrier_semaphore()
    others = [lax.rem(me + k, n) for k in range(1, n)]
    for other in others:
        pl.semaphore_signal(barrier, inc=1, device_id={"dp": other}, device_id_type=MESH)
    pl.semaphore_wait(barrier, n - 1)

    def zero(t, _):
        da[pl.ds(pl.multiple_of(t * 128, 128), 128), :] = jnp.zeros((128, d), F32)
        return 0
    lax.fori_loop(0, tokens // 128, zero, 0)
    sq[...] = jnp.zeros_like(sq)

    def turn(t, _):
        r = pl.ds(pl.multiple_of(t * sub, sub), sub)
        for c in range(chips):
            for hh in range(2):
                piece = nat[r, pl.ds((2 * c + hh) * LANES, LANES)]
                at[pl.ds(hh * half + c * LANES, LANES), r] = piece.T
        return 0

    for one in first:
        one.wait()
    lax.fori_loop(0, tokens // sub, turn, 0)
    load_h = pltpu.make_async_copy(h_ref, nat, misc.at[0])
    load_h.start()

    def remote(src, dst, ss, rs, to):
        return pltpu.make_async_remote_copy(src, dst, ss, rs, device_id={"dp": to}, device_id_type=MESH)

    def p_copy(k):
        s = lax.rem(k, SLOTS)
        return remote(out_p.at[s], in_p.at[s], p_send.at[s], p_recv.at[s], partner)

    def s1_copy(k, way):
        s = lax.rem(k, SLOTS)
        return remote(out_1.at[s, way], in_1.at[s, way], s1_send.at[s, way], s1_recv.at[s, way], (right, left)[way])

    def s2_copy(k, way):
        s = lax.rem(k, SLOTS)
        return remote(out_2.at[s, way], in_2.at[s, way], s2_send.at[s, way], s2_recv.at[s, way], (right, left)[way])

    mid = LANES // 2
    block_r, block_l, block_f = (lax.rem(chip + k, chips) for k in (1, chips - 1, 2))

    def pair_step(k):
        s = lax.rem(k, SLOTS)
        p_copy(k).wait_recv()

        @pl.when(k >= SLOTS)
        def _():
            s1_copy(k - SLOTS, 0).wait_send()
            s1_copy(k - SLOTS, 1).wait_send()
        for way in range(2):
            rows = pl.ds(way * mid, mid)
            out_1[s, way] = (own[s, block_f, rows, :] + in_p[s, block_f, rows, :].astype(F32)).astype(BF16)
        s1_copy(k, 0).start()
        s1_copy(k, 1).start()
        for block in (block_r, block_l, chip):
            own[s, block] += in_p[s, block].astype(F32)

    def pass_step(k):
        s = lax.rem(k, SLOTS)
        s1_copy(k, 0).wait_recv()
        s1_copy(k, 1).wait_recv()

        @pl.when(k >= SLOTS)
        def _():
            s2_copy(k - SLOTS, 0).wait_send()
            s2_copy(k - SLOTS, 1).wait_send()
        for way, block in ((0, block_r), (1, block_l)):
            for part in range(2):
                rows = pl.ds(part * mid, mid)
                value = own[s, block, rows, :]
                if part == way:
                    value = value + in_1[s, way].astype(F32)
                out_2[s, way, rows, :] = value.astype(BF16)
        s2_copy(k, 0).start()
        s2_copy(k, 1).start()

    def f_copy(l, j, part):
        row = j * LANES + core * mid
        row = row - (row // share) * share
        rows = pl.ds(pl.multiple_of(row, mid), mid)
        return remote(fin.at[l, j, pl.ds(part * mid, mid)], gd.at[l, rows, pl.ds(part * width, width)],
                      f_send.at[l, j, part], f_recv.at[l, j, part], partner)

    def final_step(k, kind):
        s = lax.rem(k, SLOTS)
        jj = k // 3
        l, j = layer_of(jj), lax.rem(jj, chunks)
        s2_copy(k, 0).wait_recv()
        s2_copy(k, 1).wait_recv()
        value = own[s, chip] + in_2[s, 0].astype(F32) + in_2[s, 1].astype(F32)
        value = value.astype(BF16)
        wide = value.astype(F32)
        sq[...] += jnp.sum((wide * wide).reshape(LANES // 8, 8, width), 0)
        if kind:
            to = gg if kind == 1 else gu
            for c in range(chips):
                to[l, :, pl.ds(pl.multiple_of(c * span + j * LANES, LANES), LANES)] = value[:, c * LANES:(c + 1) * LANES]
        else:
            row = j * LANES + core * mid
            owner = row // share
            local = pl.multiple_of(row - owner * share, mid)

            @pl.when(owner == core)
            def _():
                for part in range(2):
                    gd[l, pl.ds(local, mid), pl.ds(part * width, width)] = value[part * mid:(part + 1) * mid, :]

            @pl.when(owner != core)
            def _():
                fin[l, j] = value
                f_copy(l, j, 0).start()
                f_copy(l, j, 1).start()

    def store(kind, ref, s, value):
        if kind:
            for c in range(chips):
                ref[s, c] = value[c * LANES:(c + 1) * LANES, :].astype(ref.dtype)
        else:
            for c in range(chips):
                for part in range(2):
                    ref[s, c, pl.ds(part * mid, mid), :] = value[c * mid:(c + 1) * mid, part * width:(part + 1) * width].astype(ref.dtype)

    def product(kind, which):
        if kind == 0:
            rows = pl.ds(pl.multiple_of(which * (width // 2), width // 2), width // 2)
            return jnp.dot(hid_t[rows, :], ct[...], preferred_element_type=F32)
        rows = pl.ds(pl.multiple_of(which * half, half), half)
        return jnp.dot(at[rows, :], (dg if kind == 1 else du)[...], preferred_element_type=F32)

    def tick(k, kind, maybe):
        s = lax.rem(k, SLOTS)

        @pl.when(k >= SLOTS)
        def _():
            p_copy(k - SLOTS).wait_send()
        store(kind, out_p, s, product(kind, 1 - core))
        p_copy(k).start()
        store(kind, own, s, product(kind, core))

        def run(step, lag, *more):
            if maybe and lag > kind:
                pl.when(k >= lag)(lambda: step(k - lag, *more))
            else:
                step(k - lag, *more)
        run(pair_step, 1)
        run(pass_step, 2)
        run(final_step, 3, kind)

    def chunk(jj, _):
        l, slot = layer_of(jj), lax.rem(jj, 2)

        @pl.when(jj == chunks)
        def _():
            load_h.wait()

            def to_h(t, _):
                r = pl.ds(pl.multiple_of(t * 128, 128), 128)
                wide = nat[r, :].astype(F32)
                grad = da[r, :]
                scale = lax.rsqrt(jnp.mean(wide * wide, -1, keepdims=True) + 1e-6)
                back = grad * scale - wide * (scale * scale * scale * jnp.mean(grad * wide, -1, keepdims=True))
                ct[r, :] = (ct[r, :].astype(F32) + back.astype(BF16).astype(F32)).astype(BF16)
                return 0
            lax.fori_loop(0, tokens // 128, to_h, 0)
            load_a = pltpu.make_async_copy(a_ref.at[0], nat, misc.at[0])
            load_a.start()
            load_a.wait()
            lax.fori_loop(0, tokens // sub, turn, 0)

        for one in wd_loads(jj):
            one.wait()

        @pl.when(jj < chunks)
        def _():
            for one in wgu_loads(jj):
                one.wait()

        @pl.when(jj + 1 < total)
        def _():
            for one in wd_loads(jj + 1):
                one.start()

        @pl.when(jj + 1 < chunks)
        def _():
            for one in wgu_loads(jj + 1):
                one.start()

        def step(t, _):
            s = jj * tiles + t
            st = lax.rem(s, 2)
            for one in stage_loads(s):
                one.wait()

            @pl.when(s + 1 < total * tiles)
            def _():
                for one in stage_loads(s + 1):
                    one.start()
            for q in range(tile // sub):
                r = pl.ds(pl.multiple_of(t * tile + q * sub, sub), sub)
                dh[q] = lax.dot_general(ct[r, :], wd[slot], NT, preferred_element_type=F32)
                for e in range(sub // 32):
                    here = pl.ds(q * sub + e * 32, 32)
                    there = pl.ds(pl.multiple_of(t * tile + q * sub + e * 32, 32), 32)
                    gate, up = stage[st, 0, here, :], stage[st, 1, here, :]
                    back = dh[q, pl.ds(e * 32, 32), :].astype(BF16).astype(F32)
                    sig = jax.nn.sigmoid(gate)
                    silu = gate * sig
                    hid[there, :] = (silu * up).astype(BF16)
                    du[there, :] = (back * silu).astype(BF16)
                    dg[there, :] = (back * up * (sig + silu * (1.0 - sig))).astype(BF16)
                turned = hid[r, :].T
                for c in range(chips):
                    for hh in range(2):
                        hid_t[pl.ds(hh * (width // 2) + c * mid, mid), r] = turned[c * LANES + hh * mid:c * LANES + (hh + 1) * mid, :]
            return 0
        lax.fori_loop(0, tiles, step, 0)

        @pl.when(jj < chunks)
        def _():
            def back_step(t, _):
                r = pl.ds(pl.multiple_of(t * tile, tile), tile)
                da[r, :] += (lax.dot_general(dg[r, :], wgu[slot, 0], NT, preferred_element_type=F32)
                             + lax.dot_general(du[r, :], wgu[slot, 1], NT, preferred_element_type=F32))
                return 0
            lax.fori_loop(0, tiles, back_step, 0)

        for kind in range(3):
            tick(jj * 3 + kind, kind, True)
        return 0
    lax.fori_loop(0, total, chunk, 0)

    last = 3 * total
    pair_step(last - 1)
    pass_step(last - 2)
    final_step(last - 3, 0)
    pass_step(last - 1)
    final_step(last - 2, 1)
    final_step(last - 1, 2)

    squares[me] = jnp.sum(sq[...].reshape(8, width // LANES, LANES), 1)
    copies = [remote(squares.at[me], squares.at[me], q_send.at[k], q_recv.at[k], other) for k, other in enumerate(others)]
    for one in copies:
        one.start()
    outs = [pltpu.make_async_copy(a, b, misc.at[2 + i]) for i, (a, b) in enumerate(((gg, gg_out), (gu, gu_out)))]
    for one in outs:
        one.start()
    for l in range(layers):
        for j in range(chunks):
            row = j * LANES + core * mid

            @pl.when(row // share != core)
            def _():
                f_copy(l, j, 0).wait_send()
                f_copy(l, j, 1).wait_send()
            row = j * LANES + (1 - core) * mid

            @pl.when(row // share == core)
            def _():
                @pl.when(row // share != 1 - core)
                def _():
                    f_copy(l, j, 0).wait_recv()
                    f_copy(l, j, 1).wait_recv()
    outs.append(pltpu.make_async_copy(gd, gd_out, misc.at[4]))
    outs[-1].start()
    for one in copies:
        one.wait_recv()
    whole = squares[0]
    for k in range(1, n):
        whole = whole + squares[k]
    squares[n] = jnp.broadcast_to(jnp.sum(whole), (8, LANES))
    outs.append(pltpu.make_async_copy(squares.at[n], sq_out, misc.at[5]))
    outs[-1].start()
    for k in range(last - SLOTS, last):
        p_copy(k).wait_send()
        for way in range(2):
            s1_copy(k, way).wait_send()
            s2_copy(k, way).wait_send()
    for one in copies:
        one.wait_send()
    for one in outs:
        one.wait()


def backward(n, dy, g, u, dn, a, h, gate, up):
    tokens, d = dy.shape
    layers, chunks, _, width = gate.shape
    ff = g.shape[2]
    chips = n // 2
    tile = 512
    sds = jax.ShapeDtypeStruct
    dma = pltpu.SemaphoreType.DMA
    v = pltpu.VMEM
    mid = LANES // 2
    grads = [((layers, d // n, ff), BF16), ((layers, d // n, ff), BF16), ((layers, ff // n, d), BF16)]
    return pl.pallas_call(
        functools.partial(backward_kernel, n),
        name="backward",
        out_shape=tuple(sds(*g_) for g_ in grads) + (sds((8, LANES), F32),),
        in_specs=[ANY] * 8,
        out_specs=(ANY,) * 4,
        scratch_shapes=[
            v((tokens, d), BF16), v((d, tokens), BF16), v((tokens, d), BF16), v((tokens, d), F32),
            v((tokens, width), BF16), v((width, tokens), BF16), v((tokens, width), BF16), v((tokens, width), BF16),
            v((tile // 256, 256, width), F32), v((2, 2, tile, width), F32), v((2, width, d), BF16), v((2, 2, d, width), BF16),
            v((SLOTS, chips, LANES, width), F32), v((SLOTS, chips, LANES, width), BF16), v((SLOTS, chips, LANES, width), BF16),
            v((SLOTS, 2, mid, width), BF16), v((SLOTS, 2, mid, width), BF16),
            v((SLOTS, 2, LANES, width), BF16), v((SLOTS, 2, LANES, width), BF16),
            v((layers, chunks, LANES, width), BF16),
            *(v(*g_) for g_ in grads), v((8, width), F32), v((n + 1, 8, LANES), F32),
            dma((2, 2)), dma((2, chips)), dma((2, 2, chips)), dma((SLOTS,)), dma((SLOTS,)),
            dma((SLOTS, 2)), dma((SLOTS, 2)), dma((SLOTS, 2)), dma((SLOTS, 2)),
            dma((layers, chunks, 2)), dma((layers, chunks, 2)), dma((n - 1,)), dma((n - 1,)), dma((6,)),
        ],
        compiler_params=pltpu.CompilerParams(collective_id=1, has_side_effects=True, vmem_limit_bytes=60 * 1024 * 1024),
    )(dy, g, u, dn, a, h, gate, up)


def adamw(w, m, v, g):
    m = 0.9 * m + 0.1 * g
    v = 0.95 * v + 0.05 * g * g
    step = m * lax.rsqrt(v + 1e-8) + 0.1 * w
    return (w - 0.02 * step).astype(BF16), m, v


def solution(mesh):
    n = mesh.shape["dp"]

    def step(x, dy, *arrays):
        weights, m, v = (arrays[i : i + 3] for i in (0, 3, 6))
        g, u, dn, a, h, gate, up = forward(n, x[0], *weights)
        *gradients, squares = backward(n, dy[0], g, u, dn, a, h, gate, up)
        factor = jnp.minimum(1.0, 0.5 * lax.rsqrt(squares[0, 0] / (n * sum(w.size for w in weights)) + 1e-30))
        new = [adamw(w.astype(F32), m, v, g.astype(F32) * factor) for w, m, v, g in zip(weights, m, v, gradients, strict=True)]
        return tuple(one[which] for which in range(3) for one in new)

    states, cut = P(("rep", "dp"), None, None), P(None, "dp", None)
    return jax.shard_map(
        step,
        mesh=mesh,
        in_specs=(states, states) + (cut,) * 9,
        out_specs=(P("rep", "dp", None),) * 9,
        check_vma=False,
    )
```

```python
import functools

import jax
import jax.numpy as jnp
from jax import lax
from jax.experimental import pallas as pl
from jax.experimental.pallas import tpu as pltpu
from jax.sharding import PartitionSpec as P

MESH = pl.DeviceIdType.MESH
ANY = pl.BlockSpec(memory_space=pl.ANY)
F32, BF16 = jnp.float32, jnp.bfloat16
LANES = 128
NT = (((1,), (1,)), ((), ()))
TN = (((0,), (0,)), ((), ()))


def places(n):
    me = lax.axis_index("dp")
    core, chips = lax.rem(me, 2), n // 2
    chip = me // 2
    around = lambda k: lax.rem(chip + k, chips) * 2 + core
    return me, chip, core, me + 1 - 2 * core, around(1), around(chips - 1), around(2)


def greet(*others):
    barrier = pltpu.get_barrier_semaphore()
    for other in others:
        pl.semaphore_signal(barrier, inc=1, device_id={"dp": other}, device_id_type=MESH)
    pl.semaphore_wait(barrier, len(others))


def sigmoid(x):
    return 0.5 * jnp.tanh(0.5 * x) + 0.5


def norm_rows(wide):
    scale = lax.rsqrt(jnp.mean(wide * wide, -1, keepdims=True) + 1e-6)
    return (wide * scale).astype(BF16)


def forward_kernel(n, x_ref, wg_ref, wu_ref, wd_ref, g_ref, u_ref, d_ref, a_out, h_out, gate_out, up_out,
                   own_g, own_u, own_d, h, a, at, hidden, wchunk, wdown, stage,
                   send, recv, own_sem, out_sem, w_sem, stage_sem, misc):
    me, chip, core, partner, right, left, far = places(n)
    layers = wg_ref.shape[0]
    tokens, d = x_ref.shape
    chunks, _, width = gate_out.shape[1:]
    chips = n // 2
    tile = stage.shape[2]
    tiles = tokens // tile
    span = g_ref.shape[2] // chips

    order = [(l, w, o) for l in range(layers) for w, o in ((g_ref, own_g), (u_ref, own_u), (d_ref, own_d))]

    loads = [pltpu.make_async_copy(src.at[l], o.at[l], own_sem.at[3 * l + i])
             for l in range(layers) for i, (src, o) in enumerate(((wg_ref, own_g), (wu_ref, own_u), (wd_ref, own_d)))]
    for one in loads:
        one.start()
    load_x = pltpu.make_async_copy(x_ref, h, misc.at[0])
    load_x.start()
    greet(partner, right, left)

    def rows(m, device, part=None):
        l, w, o = order[m]
        count = o.shape[1]
        if part is None:
            return w.at[l, pl.ds(device * count, count)]
        return w.at[l, pl.ds(device * count + part * (count // 2), count // 2)]

    def ag(m, kind):
        l, w, o = order[m]
        src, to = [
            (None, right), (None, left),
            (rows(m, left, 0), right), (rows(m, right, 1), left),
            (None, partner), (rows(m, left), partner), (rows(m, right), partner),
            (rows(m, far, 0), partner), (rows(m, far, 1), partner),
        ][kind]
        dst = rows(m, me) if src is None else src
        return pltpu.make_async_remote_copy(o.at[l] if src is None else src, dst, send.at[m, kind], recv.at[m, kind],
                                            device_id={"dp": to}, device_id_type=MESH)

    kept = []

    def begin(m):
        loads[m].wait()
        ag(m, 0).start()
        ag(m, 1).start()
        ag(m, 4).start()
        l, w, o = order[m]
        copy = pltpu.make_async_copy(o.at[l], rows(m, me), out_sem.at[m])
        copy.start()
        kept.append(copy)

    def pass_on(m):
        ag(m, 0).wait_recv()
        ag(m, 2).start()
        ag(m, 5).start()
        ag(m, 1).wait_recv()
        ag(m, 3).start()
        ag(m, 6).start()

    def hand_over(m):
        ag(m, 2).wait_recv()
        ag(m, 7).start()
        ag(m, 3).wait_recv()
        ag(m, 8).start()

    def complete(m):
        for kind in (4, 5, 6, 7, 8):
            ag(m, kind).wait_recv()
        kept[m].wait()

    begin(0)
    begin(1)
    load_x.wait()

    def norm_step(t, _):
        r = pl.ds(pl.multiple_of(t * 256, 256), 256)
        a[r, :] = norm_rows(h[r, :].astype(F32))
        return 0
    lax.fori_loop(0, tokens // 256, norm_step, 0)

    def turn(t, _):
        r = pl.ds(pl.multiple_of(t * 256, 256), 256)
        for c in range(chips):
            for part in range(2):
                at[pl.ds(part * (d // 2) + c * LANES, LANES), r] = a[r, pl.ds((2 * c + part) * LANES, LANES)].T
        return 0
    lax.fori_loop(0, tokens // 256, turn, 0)
    a_copy = pltpu.make_async_copy(at, a_out.at[0], misc.at[1])
    a_copy.start()

    def w_loads(l, j, slot):
        return [pltpu.make_async_copy(w.at[l, :, pl.ds(c * span + j * LANES, LANES)], wchunk.at[slot, i, :, pl.ds(c * LANES, LANES)],
                                      w_sem.at[slot, i, c])
                for i, w in enumerate((g_ref, u_ref)) for c in range(chips)]

    def gate_up(l, between, with_hidden):
        for one in w_loads(l, 0, 0):
            one.start()
        for j in range(chunks):
            slot = j % 2
            for one in w_loads(l, j, slot):
                one.wait()
            if j + 1 < chunks:
                for one in w_loads(l, j + 1, 1 - slot):
                    one.start()

            def step(t, _):
                half = lax.rem(t, 2)
                r = pl.ds(pl.multiple_of(t * tile, tile), tile)

                def outs(t_):
                    rr = pl.ds(pl.multiple_of(t_ * tile, tile), tile)
                    hh = lax.rem(t_, 2)
                    return [pltpu.make_async_copy(stage.at[hh, i], o.at[l, j, rr], stage_sem.at[hh, i])
                            for i, o in enumerate((gate_out, up_out))]

                @pl.when(t >= (2 if j == 0 else 0))
                def _():
                    for one in outs(t):
                        one.wait()
                rows_a = a[r, :]
                stage[half, 0] = jnp.dot(rows_a, wchunk[slot, 0], preferred_element_type=F32)
                stage[half, 1] = jnp.dot(rows_a, wchunk[slot, 1], preferred_element_type=F32)
                if with_hidden:
                    gate, up = stage[half, 0], stage[half, 1]
                    hidden[r, pl.ds(j * width, width)] = (gate * sigmoid(gate) * up).astype(BF16)
                for one in outs(t):
                    one.start()
                return 0
            lax.fori_loop(0, tiles, step, 0)
            between(j)
        for half in range(2):
            for i, o in enumerate((gate_out, up_out)):
                pltpu.make_async_copy(stage.at[half, i], o.at[l, 0, pl.ds(0, tile)], stage_sem.at[half, i]).wait()

    pass_on(0)
    pass_on(1)
    begin(2)
    begin(3)
    hand_over(0)
    hand_over(1)
    complete(0)
    complete(1)

    def first(j):
        if j == 2:
            pass_on(2)
            begin(4)
        if j == 4:
            pass_on(3)
    gate_up(0, first, True)

    hand_over(2)
    complete(2)
    down = [pltpu.make_async_copy(d_ref.at[0, pl.ds(c * span + j * LANES, LANES)], wdown.at[pl.ds(j * width + c * LANES, LANES)], misc.at[3 + j * chips + c])
            for j in range(chunks) for c in range(chips)]
    for one in down:
        one.start()
    a_copy.wait()
    for one in down:
        one.wait()

    def down_step(t, _):
        r = pl.ds(pl.multiple_of(t * tile, tile), tile)
        y = jnp.dot(hidden[r, :], wdown[...], preferred_element_type=F32).astype(BF16)
        h1 = (h[r, :].astype(F32) + y.astype(F32)).astype(BF16)
        h[r, :] = h1
        a[r, :] = norm_rows(h1.astype(F32))
        return 0
    lax.fori_loop(0, tiles, down_step, 0)
    h_copy = pltpu.make_async_copy(h, h_out, misc.at[2])
    h_copy.start()
    pass_on(4)
    begin(5)
    lax.fori_loop(0, tokens // 256, turn, 0)
    a_copy = pltpu.make_async_copy(at, a_out.at[1], misc.at[1])
    a_copy.start()
    hand_over(3)
    hand_over(4)
    complete(3)
    complete(4)

    def second(j):
        if j == 2:
            pass_on(5)
    gate_up(1, second, False)
    hand_over(5)
    complete(5)
    h_copy.wait()
    a_copy.wait()
    for m in range(len(order)):
        for kind in range(9):
            ag(m, kind).wait_send()


def forward(n, x, wg, wu, wd):
    tokens, d = x.shape
    layers, _, ff = wg.shape
    chips = n // 2
    width = chips * LANES
    chunks = ff // width
    tile = 512
    sds = jax.ShapeDtypeStruct
    dma = pltpu.SemaphoreType.DMA
    return pl.pallas_call(
        functools.partial(forward_kernel, n),
        name="forward",
        out_shape=(
            sds((layers, d, ff), BF16), sds((layers, d, ff), BF16), sds((layers, ff, d), BF16),
            sds((layers, d, tokens), BF16), sds((tokens, d), BF16),
            sds((layers, chunks, tokens, width), F32), sds((layers, chunks, tokens, width), F32),
        ),
        in_specs=[ANY] * 4,
        out_specs=(ANY,) * 7,
        scratch_shapes=[
            pltpu.VMEM(wg.shape, BF16), pltpu.VMEM(wu.shape, BF16), pltpu.VMEM(wd.shape, BF16),
            pltpu.VMEM((tokens, d), BF16), pltpu.VMEM((tokens, d), BF16), pltpu.VMEM((d, tokens), BF16), pltpu.VMEM((tokens, ff), BF16),
            pltpu.VMEM((2, 2, d, width), BF16), pltpu.VMEM((ff, d), BF16), pltpu.VMEM((2, 2, tile, width), F32),
            dma((3 * layers, 9)), dma((3 * layers, 9)), dma((3 * layers,)), dma((3 * layers,)),
            dma((2, 2, chips)), dma((2, 2)), dma((3 + chunks * chips,)),
        ],
        compiler_params=pltpu.CompilerParams(collective_id=0, has_side_effects=True, vmem_limit_bytes=60 * 1024 * 1024),
    )(x, wg, wu, wd)


SLOTS = 6
PAIR_SLOTS = 4
AHEAD = 4
PAIR_LAG, PASS_LAG, FINAL_LAG = 1, 3, 5


def backward_kernel(n, dy_ref, g_ref, u_ref, d_ref, a_ref, h_ref, gate_ref, up_ref, gg_out, gu_out, gd_out, sq_out,
                    ct, at, hs, da, hid, hid_t, dg, du, dh, stage, wd, wgu, own, out_p, in_p, out_1, in_1, out_2, in_2, fin,
                    gg, gu, gd, sq, squares,
                    stage_sem, wd_sem, wgu_sem, h_sem, p_send, p_recv, s1_send, s1_recv, s2_send, s2_recv, f_send, f_recv, q_send, q_recv, misc):
    me, chip, core, partner, right, left, far = places(n)
    layers, chunks, tokens, width = gate_ref.shape
    d = dy_ref.shape[1]
    chips = n // 2
    span = g_ref.shape[2] // chips
    share = gd.shape[1]
    tile = stage.shape[2]
    tiles = tokens // tile
    sub = 256
    total = layers * chunks
    half = d // 2

    def layer_of(jj):
        return layers - 1 - jj // chunks

    def stage_loads(s):
        jj, t = s // tiles, lax.rem(s, tiles)
        slot = lax.rem(s, AHEAD)
        r = pl.ds(pl.multiple_of(t * tile, tile), tile)
        return [pltpu.make_async_copy(ref.at[layer_of(jj), lax.rem(jj, chunks), r], stage.at[slot, i], stage_sem.at[slot, i])
                for i, ref in enumerate((gate_ref, up_ref))]

    def wd_loads(jj):
        l, j, slot = layer_of(jj), lax.rem(jj, chunks), lax.rem(jj, 2)
        return [pltpu.make_async_copy(d_ref.at[l, pl.ds(pl.multiple_of(c * span + j * LANES, LANES), LANES)],
                                      wd.at[slot, pl.ds(c * LANES, LANES)], wd_sem.at[slot, c]) for c in range(chips)]

    def wgu_loads(jj):
        l, j, slot = layer_of(jj), lax.rem(jj, chunks), lax.rem(jj, 2)
        return [pltpu.make_async_copy(ref.at[l, :, pl.ds(pl.multiple_of(c * span + j * LANES, LANES), LANES)],
                                      wgu.at[slot, i, :, pl.ds(c * LANES, LANES)], wgu_sem.at[slot, i, c])
                for i, ref in enumerate((g_ref, u_ref)) for c in range(chips)]

    def at_load(l):
        return pltpu.make_async_copy(a_ref.at[l], at, misc.at[0])

    def h_load(t):
        slot = lax.rem(t, AHEAD)
        return pltpu.make_async_copy(h_ref.at[pl.ds(pl.multiple_of(t * sub, sub), sub)], hs.at[slot], h_sem.at[slot])

    first = [pltpu.make_async_copy(dy_ref, ct, misc.at[1])]
    for one in first + wd_loads(0) + wgu_loads(0) + [one for s in range(AHEAD) for one in stage_loads(s)]:
        one.start()
    at_load(layers - 1).start()
    for t in range(AHEAD):
        h_load(t).start()

    barrier = pltpu.get_barrier_semaphore()
    others = [lax.rem(me + k, n) for k in range(1, n)]
    for other in others:
        pl.semaphore_signal(barrier, inc=1, device_id={"dp": other}, device_id_type=MESH)

    def zero(t, _):
        da[pl.ds(pl.multiple_of(t * 128, 128), 128), :] = jnp.zeros((128, d), F32)
        return 0
    lax.fori_loop(0, tokens // 128, zero, 0)
    sq[...] = jnp.zeros_like(sq)
    pl.semaphore_wait(barrier, n - 1)
    for one in first:
        one.wait()

    def remote(src, dst, ss, rs, to):
        return pltpu.make_async_remote_copy(src, dst, ss, rs, device_id={"dp": to}, device_id_type=MESH)

    def p_copy(k):
        o, s = lax.rem(k, 2), lax.rem(k, PAIR_SLOTS)
        return remote(out_p.at[o], in_p.at[s], p_send.at[o], p_recv.at[s], partner)

    def s1_copy(k, way):
        s = lax.rem(k, SLOTS)
        return remote(out_1.at[s, way], in_1.at[s, way], s1_send.at[s, way], s1_recv.at[s, way], (right, left)[way])

    def s2_copy(k, way):
        s = lax.rem(k, SLOTS)
        return remote(out_2.at[s, way], in_2.at[s, way], s2_send.at[s, way], s2_recv.at[s, way], (right, left)[way])

    mid = LANES // 2
    block_r, block_l, block_f = (lax.rem(chip + k, chips) for k in (1, chips - 1, 2))

    def pair_step(k):
        s, p = lax.rem(k, SLOTS), lax.rem(k, PAIR_SLOTS)
        p_copy(k).wait_recv()

        @pl.when(k >= SLOTS)
        def _():
            s1_copy(k - SLOTS, 0).wait_send()
            s1_copy(k - SLOTS, 1).wait_send()
        for way in range(2):
            rows = pl.ds(way * mid, mid)
            out_1[s, way] = (own[s, block_f, rows, :] + in_p[p, block_f, rows, :].astype(F32)).astype(BF16)
        s1_copy(k, 0).start()
        s1_copy(k, 1).start()
        for block in (block_r, block_l, chip):
            own[s, block] += in_p[p, block].astype(F32)

    def pass_step(k):
        s = lax.rem(k, SLOTS)
        s1_copy(k, 0).wait_recv()
        s1_copy(k, 1).wait_recv()

        @pl.when(k >= SLOTS)
        def _():
            s2_copy(k - SLOTS, 0).wait_send()
            s2_copy(k - SLOTS, 1).wait_send()
        for way, block in ((0, block_r), (1, block_l)):
            for part in range(2):
                rows = pl.ds(part * mid, mid)
                value = own[s, block, rows, :]
                if part == way:
                    value = value + in_1[s, way].astype(F32)
                out_2[s, way, rows, :] = value.astype(BF16)
        s2_copy(k, 0).start()
        s2_copy(k, 1).start()

    def f_copy(l, j, part):
        row = j * LANES + core * mid
        row = row - (row // share) * share
        rows = pl.ds(pl.multiple_of(row, mid), mid)
        return remote(fin.at[l, j, pl.ds(part * mid, mid)], gd.at[l, rows, pl.ds(part * width, width)],
                      f_send.at[l, j, part], f_recv.at[l, j, part], partner)

    def final_step(k, kind):
        s = lax.rem(k, SLOTS)
        jj = k // 3
        l, j = layer_of(jj), lax.rem(jj, chunks)
        s2_copy(k, 0).wait_recv()
        s2_copy(k, 1).wait_recv()
        value = own[s, chip] + in_2[s, 0].astype(F32) + in_2[s, 1].astype(F32)
        value = value.astype(BF16)
        wide = value.astype(F32)
        sq[...] += jnp.sum((wide * wide).reshape(LANES // 8, 8, width), 0)
        if kind:
            to = gg if kind == 1 else gu
            for c in range(chips):
                to[l, :, pl.ds(pl.multiple_of(c * span + j * LANES, LANES), LANES)] = value[:, c * LANES:(c + 1) * LANES]
        else:
            row = j * LANES + core * mid
            owner = row // share
            local = pl.multiple_of(row - owner * share, mid)

            @pl.when(owner == core)
            def _():
                for part in range(2):
                    gd[l, pl.ds(local, mid), pl.ds(part * width, width)] = value[part * mid:(part + 1) * mid, :]

            @pl.when(owner != core)
            def _():
                fin[l, j] = value
                f_copy(l, j, 0).start()
                f_copy(l, j, 1).start()

    def store(kind, ref, s, value):
        if kind:
            for c in range(chips):
                ref[s, c] = value[c * LANES:(c + 1) * LANES, :].astype(ref.dtype)
        else:
            for c in range(chips):
                for part in range(2):
                    ref[s, c, pl.ds(part * mid, mid), :] = value[c * mid:(c + 1) * mid, part * width:(part + 1) * width].astype(ref.dtype)

    def product(kind, which):
        if kind == 0:
            rows = pl.ds(pl.multiple_of(which * (width // 2), width // 2), width // 2)
            return jnp.dot(hid_t[rows, :], ct[...], preferred_element_type=F32)
        rows = pl.ds(pl.multiple_of(which * half, half), half)
        return jnp.dot(at[rows, :], (dg if kind == 1 else du)[...], preferred_element_type=F32)

    def tick(k, kind):
        def run(step, lag, *more):
            if lag > kind:
                pl.when(k >= lag)(lambda: step(k - lag, *more))
            else:
                step(k - lag, *more)

        @pl.when(k >= 2)
        def _():
            p_copy(k - 2).wait_send()
        store(kind, out_p, lax.rem(k, 2), product(kind, 1 - core))
        p_copy(k).start()
        run(pair_step, PAIR_LAG)
        run(pass_step, PASS_LAG)
        store(kind, own, lax.rem(k, SLOTS), product(kind, core))
        run(final_step, FINAL_LAG, (kind - FINAL_LAG) % 3)

    def chunk(jj, _):
        l, slot = layer_of(jj), lax.rem(jj, 2)

        @pl.when(jj == chunks)
        def _():
            at_load(0).start()

            def to_h(t, _):
                h_load(t).wait()
                for e in range(sub // 64):
                    here = pl.ds(pl.multiple_of(t * sub + e * 64, 64), 64)
                    wide = hs[lax.rem(t, AHEAD), pl.ds(e * 64, 64), :].astype(F32)
                    grad = da[here, :]
                    scale = lax.rsqrt(jnp.mean(wide * wide, -1, keepdims=True) + 1e-6)
                    back = grad * scale - wide * (scale * scale * scale * jnp.mean(grad * wide, -1, keepdims=True))
                    ct[here, :] = (ct[here, :].astype(F32) + back).astype(BF16)

                @pl.when(t + AHEAD < tokens // sub)
                def _():
                    h_load(t + AHEAD).start()
                return 0
            lax.fori_loop(0, tokens // sub, to_h, 0)

        for one in wd_loads(jj):
            one.wait()

        @pl.when(jj < chunks)
        def _():
            for one in wgu_loads(jj):
                one.wait()

        @pl.when(jj + 1 < total)
        def _():
            for one in wd_loads(jj + 1):
                one.start()

        @pl.when(jj + 1 < chunks)
        def _():
            for one in wgu_loads(jj + 1):
                one.start()

        def step(t, _):
            s = jj * tiles + t
            st = lax.rem(s, AHEAD)
            for one in stage_loads(s):
                one.wait()
            for q in range(tile // sub):
                r = pl.ds(pl.multiple_of(t * tile + q * sub, sub), sub)
                dh[q] = lax.dot_general(ct[r, :], wd[slot], NT, preferred_element_type=F32)
                for e in range(sub // 32):
                    here = pl.ds(q * sub + e * 32, 32)
                    there = pl.ds(pl.multiple_of(t * tile + q * sub + e * 32, 32), 32)
                    gate, up = stage[st, 0, here, :], stage[st, 1, here, :]
                    back = dh[q, pl.ds(e * 32, 32), :].astype(BF16).astype(F32)
                    sig = sigmoid(gate)
                    silu = gate * sig
                    hid[q, pl.ds(e * 32, 32), :] = (silu * up).astype(BF16)
                    du[there, :] = (back * silu).astype(BF16)
                    dg[there, :] = (back * up * (sig + silu * (1.0 - sig))).astype(BF16)
                turned = hid[q].T
                for c in range(chips):
                    for hh in range(2):
                        hid_t[pl.ds(hh * (width // 2) + c * mid, mid), r] = turned[c * LANES + hh * mid:c * LANES + (hh + 1) * mid, :]

            @pl.when(s + AHEAD < total * tiles)
            def _():
                for one in stage_loads(s + AHEAD):
                    one.start()
            return 0
        lax.fori_loop(0, tiles, step, 0)

        @pl.when(lax.rem(jj, chunks) == 0)
        def _():
            at_load(layer_of(jj)).wait()

        def back(part):
            def back_step(t, _):
                r = pl.ds(pl.multiple_of(t * tile, tile), tile)
                da[r, :] += (lax.dot_general(dg[r, :], wgu[slot, 0], NT, preferred_element_type=F32)
                             + lax.dot_general(du[r, :], wgu[slot, 1], NT, preferred_element_type=F32))
                return 0

            @pl.when(jj < chunks)
            def _():
                lax.fori_loop(part * tiles // 2, (part + 1) * tiles // 2, back_step, 0)

        tick(jj * 3, 0)
        back(0)
        tick(jj * 3 + 1, 1)
        back(1)
        tick(jj * 3 + 2, 2)
        return 0
    lax.fori_loop(0, total, chunk, 0)

    last = 3 * total
    pair_step(last - 1)
    for k in range(last - PASS_LAG, last):
        pass_step(k)
        final_step(k - 2, (k - 2) % 3)
    final_step(last - 2, 1)
    final_step(last - 1, 2)

    squares[me] = jnp.sum(sq[...].reshape(8, width // LANES, LANES), 1)
    copies = [remote(squares.at[me], squares.at[me], q_send.at[k], q_recv.at[k], other) for k, other in enumerate(others)]
    for one in copies:
        one.start()
    outs = [pltpu.make_async_copy(a, b, misc.at[2 + i]) for i, (a, b) in enumerate(((gg, gg_out), (gu, gu_out)))]
    for one in outs:
        one.start()
    for l in range(layers):
        for j in range(chunks):
            row = j * LANES + core * mid

            @pl.when(row // share != core)
            def _():
                f_copy(l, j, 0).wait_send()
                f_copy(l, j, 1).wait_send()
            row = j * LANES + (1 - core) * mid

            @pl.when(row // share == core)
            def _():
                @pl.when(row // share != 1 - core)
                def _():
                    f_copy(l, j, 0).wait_recv()
                    f_copy(l, j, 1).wait_recv()
    outs.append(pltpu.make_async_copy(gd, gd_out, misc.at[4]))
    outs[-1].start()
    for one in copies:
        one.wait_recv()
    whole = squares[0]
    for k in range(1, n):
        whole = whole + squares[k]
    squares[n] = jnp.broadcast_to(jnp.sum(whole), (8, LANES))
    outs.append(pltpu.make_async_copy(squares.at[n], sq_out, misc.at[5]))
    outs[-1].start()
    for k in range(last - 2, last):
        p_copy(k).wait_send()
    for k in range(last - SLOTS, last):
        for way in range(2):
            s1_copy(k, way).wait_send()
            s2_copy(k, way).wait_send()
    for one in copies:
        one.wait_send()
    for one in outs:
        one.wait()


def backward(n, dy, g, u, dn, a, h, gate, up):
    tokens, d = dy.shape
    layers, chunks, _, width = gate.shape
    ff = g.shape[2]
    chips = n // 2
    tile = 512
    sds = jax.ShapeDtypeStruct
    dma = pltpu.SemaphoreType.DMA
    v = pltpu.VMEM
    mid = LANES // 2
    grads = [((layers, d // n, ff), BF16), ((layers, d // n, ff), BF16), ((layers, ff // n, d), BF16)]
    return pl.pallas_call(
        functools.partial(backward_kernel, n),
        name="backward",
        out_shape=tuple(sds(*g_) for g_ in grads) + (sds((8, LANES), F32),),
        in_specs=[ANY] * 8,
        out_specs=(ANY,) * 4,
        scratch_shapes=[
            v((tokens, d), BF16), v((d, tokens), BF16), v((AHEAD, 256, d), BF16), v((tokens, d), F32),
            v((tile // 256, 256, width), BF16), v((width, tokens), BF16), v((tokens, width), BF16), v((tokens, width), BF16),
            v((tile // 256, 256, width), F32), v((AHEAD, 2, tile, width), F32), v((2, width, d), BF16), v((2, 2, d, width), BF16),
            v((SLOTS, chips, LANES, width), F32), v((2, chips, LANES, width), BF16), v((PAIR_SLOTS, chips, LANES, width), BF16),
            v((SLOTS, 2, mid, width), BF16), v((SLOTS, 2, mid, width), BF16),
            v((SLOTS, 2, LANES, width), BF16), v((SLOTS, 2, LANES, width), BF16),
            v((layers, chunks, LANES, width), BF16),
            *(v(*g_) for g_ in grads), v((8, width), F32), v((n + 1, 8, LANES), F32),
            dma((AHEAD, 2)), dma((2, chips)), dma((2, 2, chips)), dma((AHEAD,)), dma((2,)), dma((PAIR_SLOTS,)),
            dma((SLOTS, 2)), dma((SLOTS, 2)), dma((SLOTS, 2)), dma((SLOTS, 2)),
            dma((layers, chunks, 2)), dma((layers, chunks, 2)), dma((n - 1,)), dma((n - 1,)), dma((6,)),
        ],
        compiler_params=pltpu.CompilerParams(collective_id=1, has_side_effects=True, vmem_limit_bytes=60 * 1024 * 1024),
    )(dy, g, u, dn, a, h, gate, up)


def adamw(w, m, v, g):
    m = 0.9 * m + 0.1 * g
    v = 0.95 * v + 0.05 * g * g
    step = m * lax.rsqrt(v + 1e-8) + 0.1 * w
    return (w - 0.02 * step).astype(BF16), m, v


def solution(mesh):
    n = mesh.shape["dp"]

    def step(x, dy, *arrays):
        weights, m, v = (arrays[i : i + 3] for i in (0, 3, 6))
        g, u, dn, a, h, gate, up = forward(n, x[0], *weights)
        *gradients, squares = backward(n, dy[0], g, u, dn, a, h, gate, up)
        factor = jnp.minimum(1.0, 0.5 * lax.rsqrt(squares[0, 0] / (n * sum(w.size for w in weights)) + 1e-30))
        new = [adamw(w.astype(F32), m, v, g.astype(F32) * factor) for w, m, v, g in zip(weights, m, v, gradients, strict=True)]
        return tuple(one[which] for which in range(3) for one in new)

    states, cut = P(("rep", "dp"), None, None), P(None, "dp", None)
    return jax.shard_map(
        step,
        mesh=mesh,
        in_specs=(states, states) + (cut,) * 9,
        out_specs=(P("rep", "dp", None),) * 9,
        check_vma=False,
    )
```

```python
import functools

import jax
import jax.numpy as jnp
from jax import lax
from jax.experimental import pallas as pl
from jax.experimental.pallas import tpu as pltpu
from jax.sharding import PartitionSpec as P

MESH = pl.DeviceIdType.MESH
ANY = pl.BlockSpec(memory_space=pl.ANY)
F32, BF16 = jnp.float32, jnp.bfloat16
LANES = 128
NT = (((1,), (1,)), ((), ()))
TN = (((0,), (0,)), ((), ()))


def places(n):
    me = lax.axis_index("dp")
    core, chips = lax.rem(me, 2), n // 2
    chip = me // 2
    around = lambda k: lax.rem(chip + k, chips) * 2 + core
    return me, chip, core, me + 1 - 2 * core, around(1), around(chips - 1), around(2)


def greet(*others):
    barrier = pltpu.get_barrier_semaphore()
    for other in others:
        pl.semaphore_signal(barrier, inc=1, device_id={"dp": other}, device_id_type=MESH)
    pl.semaphore_wait(barrier, len(others))


def sigmoid(x):
    return 0.5 * jnp.tanh(0.5 * x) + 0.5


def norm_rows(wide):
    scale = lax.rsqrt(jnp.mean(wide * wide, -1, keepdims=True) + 1e-6)
    return (wide * scale).astype(BF16)


def forward_kernel(n, x_ref, wg_ref, wu_ref, wd_ref, g_ref, u_ref, d_ref, a_out, h_out, gate_out, up_out, hid_out,
                   own_g, own_u, own_d, h, a, at, hidden, wchunk, wdown, stage, hid, hid_t,
                   send, recv, own_sem, out_sem, w_sem, stage_sem, hid_sem, misc):
    me, chip, core, partner, right, left, far = places(n)
    layers = wg_ref.shape[0]
    tokens, d = x_ref.shape
    chunks, _, width = gate_out.shape[1:]
    chips = n // 2
    tile = stage.shape[2]
    tiles = tokens // tile
    span = g_ref.shape[2] // chips

    order = [(l, w, o) for l in range(layers) for w, o in ((g_ref, own_g), (u_ref, own_u), (d_ref, own_d))]

    loads = [pltpu.make_async_copy(src.at[l], o.at[l], own_sem.at[3 * l + i])
             for l in range(layers) for i, (src, o) in enumerate(((wg_ref, own_g), (wu_ref, own_u), (wd_ref, own_d)))]
    for one in loads:
        one.start()
    load_x = pltpu.make_async_copy(x_ref, h, misc.at[0])
    load_x.start()
    greet(partner, right, left)

    def rows(m, device, part=None):
        l, w, o = order[m]
        count = o.shape[1]
        if part is None:
            return w.at[l, pl.ds(device * count, count)]
        return w.at[l, pl.ds(device * count + part * (count // 2), count // 2)]

    def ag(m, kind):
        l, w, o = order[m]
        src, to = [
            (None, right), (None, left),
            (rows(m, left, 0), right), (rows(m, right, 1), left),
            (None, partner), (rows(m, left), partner), (rows(m, right), partner),
            (rows(m, far, 0), partner), (rows(m, far, 1), partner),
        ][kind]
        dst = rows(m, me) if src is None else src
        return pltpu.make_async_remote_copy(o.at[l] if src is None else src, dst, send.at[m, kind], recv.at[m, kind],
                                            device_id={"dp": to}, device_id_type=MESH)

    kept = []

    def begin(m):
        loads[m].wait()
        ag(m, 0).start()
        ag(m, 1).start()
        ag(m, 4).start()
        l, w, o = order[m]
        copy = pltpu.make_async_copy(o.at[l], rows(m, me), out_sem.at[m])
        copy.start()
        kept.append(copy)

    def pass_on(m):
        ag(m, 0).wait_recv()
        ag(m, 2).start()
        ag(m, 5).start()
        ag(m, 1).wait_recv()
        ag(m, 3).start()
        ag(m, 6).start()

    def hand_over(m):
        ag(m, 2).wait_recv()
        ag(m, 7).start()
        ag(m, 3).wait_recv()
        ag(m, 8).start()

    def complete(m):
        for kind in (4, 5, 6, 7, 8):
            ag(m, kind).wait_recv()
        kept[m].wait()

    begin(0)
    begin(1)
    load_x.wait()

    def norm_step(t, _):
        r = pl.ds(pl.multiple_of(t * 256, 256), 256)
        a[r, :] = norm_rows(h[r, :].astype(F32))
        return 0
    lax.fori_loop(0, tokens // 256, norm_step, 0)

    def turn(t, _):
        r = pl.ds(pl.multiple_of(t * 256, 256), 256)
        for c in range(chips):
            for part in range(2):
                at[pl.ds(part * (d // 2) + c * LANES, LANES), r] = a[r, pl.ds((2 * c + part) * LANES, LANES)].T
        return 0
    lax.fori_loop(0, tokens // 256, turn, 0)
    a_copy = pltpu.make_async_copy(at, a_out.at[0], misc.at[1])
    a_copy.start()

    def w_loads(l, j, slot):
        return [pltpu.make_async_copy(w.at[l, :, pl.ds(c * span + j * LANES, LANES)], wchunk.at[slot, i, :, pl.ds(c * LANES, LANES)],
                                      w_sem.at[slot, i, c])
                for i, w in enumerate((g_ref, u_ref)) for c in range(chips)]

    def gate_up(l, between, with_hidden):
        for one in w_loads(l, 0, 0):
            one.start()
        for j in range(chunks):
            slot = j % 2
            for one in w_loads(l, j, slot):
                one.wait()
            if j + 1 < chunks:
                for one in w_loads(l, j + 1, 1 - slot):
                    one.start()

            def step(t, _):
                half = lax.rem(t, 2)
                r = pl.ds(pl.multiple_of(t * tile, tile), tile)

                def outs(t_):
                    rr = pl.ds(pl.multiple_of(t_ * tile, tile), tile)
                    hh = lax.rem(t_, 2)
                    return [pltpu.make_async_copy(stage.at[hh, i], o.at[l, j, rr], stage_sem.at[hh, i])
                            for i, o in enumerate((gate_out, up_out))]

                @pl.when(t >= (2 if j == 0 else 0))
                def _():
                    for one in outs(t):
                        one.wait()
                for q in range(tile // 256):
                    rows_a = a[pl.ds(pl.multiple_of(t * tile + q * 256, 256), 256), :]
                    for i in range(2):
                        stage[half, i, pl.ds(q * 256, 256), :] = jnp.dot(rows_a, wchunk[slot, i], preferred_element_type=F32)
                    for e in range(256 // 32):
                        here = pl.ds(q * 256 + e * 32, 32)
                        gate, up = stage[half, 0, here, :], stage[half, 1, here, :]
                        sig = sigmoid(gate)
                        silu = gate * sig
                        value = (silu * up).astype(BF16)
                        hid[q, pl.ds(e * 32, 32), :] = value
                        if with_hidden:
                            hidden[pl.ds(pl.multiple_of(t * tile + q * 256 + e * 32, 32), 32), pl.ds(j * width, width)] = value
                        stage[half, 0, here, :] = silu
                        stage[half, 1, here, :] = up * (sig + silu * (1.0 - sig))
                    turned = hid[q].T
                    to = pl.ds(pl.multiple_of(t * tile + q * 256, 256), 256)
                    for c in range(chips):
                        for hh in range(2):
                            hid_t[slot, pl.ds(hh * (width // 2) + c * (LANES // 2), LANES // 2), to] = \
                                turned[c * LANES + hh * (LANES // 2):c * LANES + (hh + 1) * (LANES // 2), :]
                for one in outs(t):
                    one.start()
                return 0
            if j >= 2:
                pltpu.make_async_copy(hid_t.at[slot], hid_out.at[l, j], hid_sem.at[slot]).wait()
            lax.fori_loop(0, tiles, step, 0)
            pltpu.make_async_copy(hid_t.at[slot], hid_out.at[l, j], hid_sem.at[slot]).start()
            between(j)
        for slot in range(2):
            pltpu.make_async_copy(hid_t.at[slot], hid_out.at[l, 0], hid_sem.at[slot]).wait()
        for half in range(2):
            for i, o in enumerate((gate_out, up_out)):
                pltpu.make_async_copy(stage.at[half, i], o.at[l, 0, pl.ds(0, tile)], stage_sem.at[half, i]).wait()

    pass_on(0)
    pass_on(1)
    begin(2)
    begin(3)
    hand_over(0)
    hand_over(1)
    complete(0)
    complete(1)

    def first(j):
        if j == 2:
            pass_on(2)
            begin(4)
        if j == 4:
            pass_on(3)
    gate_up(0, first, True)

    hand_over(2)
    complete(2)
    down = [pltpu.make_async_copy(d_ref.at[0, pl.ds(c * span + j * LANES, LANES)], wdown.at[pl.ds(j * width + c * LANES, LANES)], misc.at[3 + j * chips + c])
            for j in range(chunks) for c in range(chips)]
    for one in down:
        one.start()
    a_copy.wait()
    for one in down:
        one.wait()

    def down_step(t, _):
        r = pl.ds(pl.multiple_of(t * tile, tile), tile)
        y = jnp.dot(hidden[r, :], wdown[...], preferred_element_type=F32).astype(BF16)
        h1 = (h[r, :].astype(F32) + y.astype(F32)).astype(BF16)
        h[r, :] = h1
        a[r, :] = norm_rows(h1.astype(F32))
        return 0
    lax.fori_loop(0, tiles, down_step, 0)
    h_copy = pltpu.make_async_copy(h, h_out, misc.at[2])
    h_copy.start()
    pass_on(4)
    begin(5)
    lax.fori_loop(0, tokens // 256, turn, 0)
    a_copy = pltpu.make_async_copy(at, a_out.at[1], misc.at[1])
    a_copy.start()
    hand_over(3)
    hand_over(4)
    complete(3)
    complete(4)

    def second(j):
        if j == 2:
            pass_on(5)
    gate_up(1, second, False)
    hand_over(5)
    complete(5)
    h_copy.wait()
    a_copy.wait()
    for m in range(len(order)):
        for kind in range(9):
            ag(m, kind).wait_send()


def forward(n, x, wg, wu, wd):
    tokens, d = x.shape
    layers, _, ff = wg.shape
    chips = n // 2
    width = chips * LANES
    chunks = ff // width
    tile = 512
    sds = jax.ShapeDtypeStruct
    dma = pltpu.SemaphoreType.DMA
    return pl.pallas_call(
        functools.partial(forward_kernel, n),
        name="forward",
        out_shape=(
            sds((layers, d, ff), BF16), sds((layers, d, ff), BF16), sds((layers, ff, d), BF16),
            sds((layers, d, tokens), BF16), sds((tokens, d), BF16),
            sds((layers, chunks, tokens, width), F32), sds((layers, chunks, tokens, width), F32),
            sds((layers, chunks, width, tokens), BF16),
        ),
        in_specs=[ANY] * 4,
        out_specs=(ANY,) * 8,
        scratch_shapes=[
            pltpu.VMEM(wg.shape, BF16), pltpu.VMEM(wu.shape, BF16), pltpu.VMEM(wd.shape, BF16),
            pltpu.VMEM((tokens, d), BF16), pltpu.VMEM((tokens, d), BF16), pltpu.VMEM((d, tokens), BF16), pltpu.VMEM((tokens, ff), BF16),
            pltpu.VMEM((2, 2, d, width), BF16), pltpu.VMEM((ff, d), BF16), pltpu.VMEM((2, 2, tile, width), F32),
            pltpu.VMEM((tile // 256, 256, width), BF16), pltpu.VMEM((2, width, tokens), BF16),
            dma((3 * layers, 9)), dma((3 * layers, 9)), dma((3 * layers,)), dma((3 * layers,)),
            dma((2, 2, chips)), dma((2, 2)), dma((2,)), dma((3 + chunks * chips,)),
        ],
        compiler_params=pltpu.CompilerParams(collective_id=0, has_side_effects=True, vmem_limit_bytes=60 * 1024 * 1024),
    )(x, wg, wu, wd)


SLOTS = 6
PAIR_SLOTS = 4
AHEAD = 4
PAIR_LAG, PASS_LAG, FINAL_LAG = 1, 3, 5


def backward_kernel(n, dy_ref, g_ref, u_ref, d_ref, a_ref, h_ref, gate_ref, up_ref, hid_ref, gg_out, gu_out, gd_out, sq_out,
                    ct, at, hs, da, hid_t, dg, du, dh, stage, wd, wgu, own, out_p, in_p, out_1, in_1, out_2, in_2, fin,
                    gg, gu, gd, sq, squares,
                    stage_sem, wd_sem, wgu_sem, h_sem, p_send, p_recv, s1_send, s1_recv, s2_send, s2_recv, f_send, f_recv, q_send, q_recv, misc):
    me, chip, core, partner, right, left, far = places(n)
    layers, chunks, tokens, width = gate_ref.shape
    d = dy_ref.shape[1]
    chips = n // 2
    span = g_ref.shape[2] // chips
    share = gd.shape[1]
    tile = stage.shape[2]
    tiles = tokens // tile
    sub = 256
    total = layers * chunks
    half = d // 2

    def layer_of(jj):
        return layers - 1 - jj // chunks

    def stage_loads(s):
        jj, t = s // tiles, lax.rem(s, tiles)
        slot = lax.rem(s, AHEAD)
        r = pl.ds(pl.multiple_of(t * tile, tile), tile)
        return [pltpu.make_async_copy(ref.at[layer_of(jj), lax.rem(jj, chunks), r], stage.at[slot, i], stage_sem.at[slot, i])
                for i, ref in enumerate((gate_ref, up_ref))]

    def wd_loads(jj):
        l, j, slot = layer_of(jj), lax.rem(jj, chunks), lax.rem(jj, 2)
        return [pltpu.make_async_copy(d_ref.at[l, pl.ds(pl.multiple_of(c * span + j * LANES, LANES), LANES)],
                                      wd.at[slot, pl.ds(c * LANES, LANES)], wd_sem.at[slot, c]) for c in range(chips)]

    def wgu_loads(jj):
        l, j, slot = layer_of(jj), lax.rem(jj, chunks), lax.rem(jj, 2)
        return [pltpu.make_async_copy(ref.at[l, :, pl.ds(pl.multiple_of(c * span + j * LANES, LANES), LANES)],
                                      wgu.at[slot, i, :, pl.ds(c * LANES, LANES)], wgu_sem.at[slot, i, c])
                for i, ref in enumerate((g_ref, u_ref)) for c in range(chips)]

    def at_load(l):
        return pltpu.make_async_copy(a_ref.at[l], at, misc.at[0])

    def h_load(t):
        slot = lax.rem(t, AHEAD)
        return pltpu.make_async_copy(h_ref.at[pl.ds(pl.multiple_of(t * sub, sub), sub)], hs.at[slot], h_sem.at[slot])

    def hid_load(jj):
        return pltpu.make_async_copy(hid_ref.at[layer_of(jj), lax.rem(jj, chunks)], hid_t, misc.at[2])

    first = [pltpu.make_async_copy(dy_ref, ct, misc.at[1])]
    for one in first + wd_loads(0) + stage_loads(0) + stage_loads(1):
        one.start()

    barrier = pltpu.get_barrier_semaphore()
    others = [lax.rem(me + k, n) for k in range(1, n)]
    for other in others:
        pl.semaphore_signal(barrier, inc=1, device_id={"dp": other}, device_id_type=MESH)

    def zero(t, _):
        da[pl.ds(pl.multiple_of(t * 128, 128), 128), :] = jnp.zeros((128, d), F32)
        return 0
    lax.fori_loop(0, tokens // 128, zero, 0)
    sq[...] = jnp.zeros_like(sq)
    pl.semaphore_wait(barrier, n - 1)
    for one in first:
        one.wait()
    for one in stage_loads(2) + stage_loads(3) + [hid_load(0)] + wgu_loads(0):
        one.start()
    at_load(layers - 1).start()
    for t in range(AHEAD):
        h_load(t).start()

    def remote(src, dst, ss, rs, to):
        return pltpu.make_async_remote_copy(src, dst, ss, rs, device_id={"dp": to}, device_id_type=MESH)

    def p_copy(k):
        o, s = lax.rem(k, 2), lax.rem(k, PAIR_SLOTS)
        return remote(out_p.at[o], in_p.at[s], p_send.at[o], p_recv.at[s], partner)

    def s1_copy(k, way):
        s = lax.rem(k, SLOTS)
        return remote(out_1.at[s, way], in_1.at[s, way], s1_send.at[s, way], s1_recv.at[s, way], (right, left)[way])

    def s2_copy(k, way):
        s = lax.rem(k, SLOTS)
        return remote(out_2.at[s, way], in_2.at[s, way], s2_send.at[s, way], s2_recv.at[s, way], (right, left)[way])

    mid = LANES // 2
    block_r, block_l, block_f = (lax.rem(chip + k, chips) for k in (1, chips - 1, 2))

    def pair_step(k):
        s, p = lax.rem(k, SLOTS), lax.rem(k, PAIR_SLOTS)
        p_copy(k).wait_recv()

        @pl.when(k >= SLOTS)
        def _():
            s1_copy(k - SLOTS, 0).wait_send()
            s1_copy(k - SLOTS, 1).wait_send()
        for way in range(2):
            rows = pl.ds(way * mid, mid)
            out_1[s, way] = (own[s, block_f, rows, :] + in_p[p, block_f, rows, :].astype(F32)).astype(BF16)
        s1_copy(k, 0).start()
        s1_copy(k, 1).start()
        for block in (block_r, block_l, chip):
            own[s, block] += in_p[p, block].astype(F32)

    def pass_step(k):
        s = lax.rem(k, SLOTS)
        s1_copy(k, 0).wait_recv()
        s1_copy(k, 1).wait_recv()

        @pl.when(k >= SLOTS)
        def _():
            s2_copy(k - SLOTS, 0).wait_send()
            s2_copy(k - SLOTS, 1).wait_send()
        for way, block in ((0, block_r), (1, block_l)):
            for part in range(2):
                rows = pl.ds(part * mid, mid)
                value = own[s, block, rows, :]
                if part == way:
                    value = value + in_1[s, way].astype(F32)
                out_2[s, way, rows, :] = value.astype(BF16)
        s2_copy(k, 0).start()
        s2_copy(k, 1).start()

    def f_copy(l, j, part):
        row = j * LANES + core * mid
        row = row - (row // share) * share
        rows = pl.ds(pl.multiple_of(row, mid), mid)
        return remote(fin.at[l, j, pl.ds(part * mid, mid)], gd.at[l, rows, pl.ds(part * width, width)],
                      f_send.at[l, j, part], f_recv.at[l, j, part], partner)

    def final_step(k, kind):
        s = lax.rem(k, SLOTS)
        jj = k // 3
        l, j = layer_of(jj), lax.rem(jj, chunks)
        s2_copy(k, 0).wait_recv()
        s2_copy(k, 1).wait_recv()
        value = own[s, chip] + in_2[s, 0].astype(F32) + in_2[s, 1].astype(F32)
        value = value.astype(BF16)
        wide = value.astype(F32)
        sq[...] += jnp.sum((wide * wide).reshape(LANES // 8, 8, width), 0)
        if kind:
            to = gg if kind == 1 else gu
            for c in range(chips):
                to[l, :, pl.ds(pl.multiple_of(c * span + j * LANES, LANES), LANES)] = value[:, c * LANES:(c + 1) * LANES]
        else:
            row = j * LANES + core * mid
            owner = row // share
            local = pl.multiple_of(row - owner * share, mid)

            @pl.when(owner == core)
            def _():
                for part in range(2):
                    gd[l, pl.ds(local, mid), pl.ds(part * width, width)] = value[part * mid:(part + 1) * mid, :]

            @pl.when(owner != core)
            def _():
                fin[l, j] = value
                f_copy(l, j, 0).start()
                f_copy(l, j, 1).start()

    def store(kind, ref, s, value):
        if kind:
            for c in range(chips):
                ref[s, c] = value[c * LANES:(c + 1) * LANES, :].astype(ref.dtype)
        else:
            for c in range(chips):
                for part in range(2):
                    ref[s, c, pl.ds(part * mid, mid), :] = value[c * mid:(c + 1) * mid, part * width:(part + 1) * width].astype(ref.dtype)

    def product(kind, which):
        if kind == 0:
            rows = pl.ds(pl.multiple_of(which * (width // 2), width // 2), width // 2)
            return jnp.dot(hid_t[rows, :], ct[...], preferred_element_type=F32)
        rows = pl.ds(pl.multiple_of(which * half, half), half)
        return jnp.dot(at[rows, :], (dg if kind == 1 else du)[...], preferred_element_type=F32)

    def tick(k, kind):
        def run(step, lag, *more):
            if lag > kind:
                pl.when(k >= lag)(lambda: step(k - lag, *more))
            else:
                step(k - lag, *more)

        @pl.when(k >= 2)
        def _():
            p_copy(k - 2).wait_send()
        store(kind, out_p, lax.rem(k, 2), product(kind, 1 - core))
        p_copy(k).start()
        run(pair_step, PAIR_LAG)
        run(pass_step, PASS_LAG)
        store(kind, own, lax.rem(k, SLOTS), product(kind, core))
        run(final_step, FINAL_LAG, (kind - FINAL_LAG) % 3)

    def chunk(jj, _):
        l, slot = layer_of(jj), lax.rem(jj, 2)

        @pl.when(jj == chunks)
        def _():
            at_load(0).start()

            def to_h(t, _):
                h_load(t).wait()
                for e in range(sub // 64):
                    here = pl.ds(pl.multiple_of(t * sub + e * 64, 64), 64)
                    wide = hs[lax.rem(t, AHEAD), pl.ds(e * 64, 64), :].astype(F32)
                    grad = da[here, :]
                    scale = lax.rsqrt(jnp.mean(wide * wide, -1, keepdims=True) + 1e-6)
                    back = grad * scale - wide * (scale * scale * scale * jnp.mean(grad * wide, -1, keepdims=True))
                    ct[here, :] = (ct[here, :].astype(F32) + back).astype(BF16)

                @pl.when(t + AHEAD < tokens // sub)
                def _():
                    h_load(t + AHEAD).start()
                return 0
            lax.fori_loop(0, tokens // sub, to_h, 0)

        for one in wd_loads(jj):
            one.wait()

        @pl.when(jj + 1 < total)
        def _():
            for one in wd_loads(jj + 1):
                one.start()

        @pl.when(jj + 1 < chunks)
        def _():
            for one in wgu_loads(jj + 1):
                one.start()

        def step(t, _):
            s = jj * tiles + t
            st = lax.rem(s, AHEAD)
            for one in stage_loads(s):
                one.wait()
            for q in range(tile // sub):
                r = pl.ds(pl.multiple_of(t * tile + q * sub, sub), sub)
                dh[q] = lax.dot_general(ct[r, :], wd[slot], NT, preferred_element_type=F32)
                for e in range(sub // 32):
                    here = pl.ds(q * sub + e * 32, 32)
                    there = pl.ds(pl.multiple_of(t * tile + q * sub + e * 32, 32), 32)
                    back = dh[q, pl.ds(e * 32, 32), :].astype(BF16).astype(F32)
                    du[there, :] = (back * stage[st, 0, here, :]).astype(BF16)
                    dg[there, :] = (back * stage[st, 1, here, :]).astype(BF16)

            @pl.when(s + AHEAD < total * tiles)
            def _():
                for one in stage_loads(s + AHEAD):
                    one.start()
            return 0
        lax.fori_loop(0, tiles, step, 0)

        @pl.when(lax.rem(jj, chunks) == 0)
        def _():
            at_load(layer_of(jj)).wait()

        def back(part):
            def back_step(t, _):
                r = pl.ds(pl.multiple_of(t * tile, tile), tile)
                da[r, :] += (lax.dot_general(dg[r, :], wgu[slot, 0], NT, preferred_element_type=F32)
                             + lax.dot_general(du[r, :], wgu[slot, 1], NT, preferred_element_type=F32))
                return 0

            @pl.when(jj < chunks)
            def _():
                lax.fori_loop(part * tiles // 2, (part + 1) * tiles // 2, back_step, 0)

        hid_load(jj).wait()
        tick(jj * 3, 0)

        @pl.when(jj + 1 < total)
        def _():
            hid_load(jj + 1).start()

        @pl.when(jj < chunks)
        def _():
            for one in wgu_loads(jj):
                one.wait()
        back(0)
        tick(jj * 3 + 1, 1)
        back(1)
        tick(jj * 3 + 2, 2)
        return 0
    lax.fori_loop(0, total, chunk, 0)

    last = 3 * total
    pair_step(last - 1)
    for k in range(last - PASS_LAG, last):
        pass_step(k)
        final_step(k - 2, (k - 2) % 3)
    final_step(last - 2, 1)
    final_step(last - 1, 2)

    squares[me] = jnp.sum(sq[...].reshape(8, width // LANES, LANES), 1)
    copies = [remote(squares.at[me], squares.at[me], q_send.at[k], q_recv.at[k], other) for k, other in enumerate(others)]
    for one in copies:
        one.start()
    outs = [pltpu.make_async_copy(a, b, misc.at[3 + i]) for i, (a, b) in enumerate(((gg, gg_out), (gu, gu_out)))]
    for one in outs:
        one.start()
    for l in range(layers):
        for j in range(chunks):
            row = j * LANES + core * mid

            @pl.when(row // share != core)
            def _():
                f_copy(l, j, 0).wait_send()
                f_copy(l, j, 1).wait_send()
            row = j * LANES + (1 - core) * mid

            @pl.when(row // share == core)
            def _():
                @pl.when(row // share != 1 - core)
                def _():
                    f_copy(l, j, 0).wait_recv()
                    f_copy(l, j, 1).wait_recv()
    outs.append(pltpu.make_async_copy(gd, gd_out, misc.at[5]))
    outs[-1].start()
    for one in copies:
        one.wait_recv()
    whole = squares[0]
    for k in range(1, n):
        whole = whole + squares[k]
    squares[n] = jnp.broadcast_to(jnp.sum(whole), (8, LANES))
    outs.append(pltpu.make_async_copy(squares.at[n], sq_out, misc.at[6]))
    outs[-1].start()
    for k in range(last - 2, last):
        p_copy(k).wait_send()
    for k in range(last - SLOTS, last):
        for way in range(2):
            s1_copy(k, way).wait_send()
            s2_copy(k, way).wait_send()
    for one in copies:
        one.wait_send()
    for one in outs:
        one.wait()


def backward(n, dy, g, u, dn, a, h, gate, up, hid):
    tokens, d = dy.shape
    layers, chunks, _, width = gate.shape
    ff = g.shape[2]
    chips = n // 2
    tile = 512
    sds = jax.ShapeDtypeStruct
    dma = pltpu.SemaphoreType.DMA
    v = pltpu.VMEM
    mid = LANES // 2
    grads = [((layers, d // n, ff), BF16), ((layers, d // n, ff), BF16), ((layers, ff // n, d), BF16)]
    return pl.pallas_call(
        functools.partial(backward_kernel, n),
        name="backward",
        out_shape=tuple(sds(*g_) for g_ in grads) + (sds((8, LANES), F32),),
        in_specs=[ANY] * 9,
        out_specs=(ANY,) * 4,
        scratch_shapes=[
            v((tokens, d), BF16), v((d, tokens), BF16), v((AHEAD, 256, d), BF16), v((tokens, d), F32),
            v((width, tokens), BF16), v((tokens, width), BF16), v((tokens, width), BF16),
            v((tile // 256, 256, width), F32), v((AHEAD, 2, tile, width), F32), v((2, width, d), BF16), v((2, 2, d, width), BF16),
            v((SLOTS, chips, LANES, width), F32), v((2, chips, LANES, width), BF16), v((PAIR_SLOTS, chips, LANES, width), BF16),
            v((SLOTS, 2, mid, width), BF16), v((SLOTS, 2, mid, width), BF16),
            v((SLOTS, 2, LANES, width), BF16), v((SLOTS, 2, LANES, width), BF16),
            v((layers, chunks, LANES, width), BF16),
            *(v(*g_) for g_ in grads), v((8, width), F32), v((n + 1, 8, LANES), F32),
            dma((AHEAD, 2)), dma((2, chips)), dma((2, 2, chips)), dma((AHEAD,)), dma((2,)), dma((PAIR_SLOTS,)),
            dma((SLOTS, 2)), dma((SLOTS, 2)), dma((SLOTS, 2)), dma((SLOTS, 2)),
            dma((layers, chunks, 2)), dma((layers, chunks, 2)), dma((n - 1,)), dma((n - 1,)), dma((7,)),
        ],
        compiler_params=pltpu.CompilerParams(collective_id=1, has_side_effects=True, vmem_limit_bytes=60 * 1024 * 1024),
    )(dy, g, u, dn, a, h, gate, up, hid)


def adamw(w, m, v, g):
    m = 0.9 * m + 0.1 * g
    v = 0.95 * v + 0.05 * g * g
    step = m * lax.rsqrt(v + 1e-8) + 0.1 * w
    return (w - 0.02 * step).astype(BF16), m, v


def solution(mesh):
    n = mesh.shape["dp"]

    def step(x, dy, *arrays):
        weights, m, v = (arrays[i : i + 3] for i in (0, 3, 6))
        g, u, dn, *saved = forward(n, x[0], *weights)
        *gradients, squares = backward(n, dy[0], g, u, dn, *saved)
        factor = jnp.minimum(1.0, 0.5 * lax.rsqrt(squares[0, 0] / (n * sum(w.size for w in weights)) + 1e-30))
        new = [adamw(w.astype(F32), m, v, g.astype(F32) * factor) for w, m, v, g in zip(weights, m, v, gradients, strict=True)]
        return tuple(one[which] for which in range(3) for one in new)

    states, cut = P(("rep", "dp"), None, None), P(None, "dp", None)
    return jax.shard_map(
        step,
        mesh=mesh,
        in_specs=(states, states) + (cut,) * 9,
        out_specs=(P("rep", "dp", None),) * 9,
        check_vma=False,
    )
```

```python
import functools

import jax
import jax.numpy as jnp
from jax import lax
from jax.experimental import pallas as pl
from jax.experimental.pallas import tpu as pltpu
from jax.sharding import PartitionSpec as P

MESH = pl.DeviceIdType.MESH
ANY = pl.BlockSpec(memory_space=pl.ANY)
F32, BF16 = jnp.float32, jnp.bfloat16
LANES = 128
NT = (((1,), (1,)), ((), ()))
TN = (((0,), (0,)), ((), ()))


def places(n):
    me = lax.axis_index("dp")
    core, chips = lax.rem(me, 2), n // 2
    chip = me // 2
    around = lambda k: lax.rem(chip + k, chips) * 2 + core
    return me, chip, core, me + 1 - 2 * core, around(1), around(chips - 1), around(2)


def greet(*others):
    barrier = pltpu.get_barrier_semaphore()
    for other in others:
        pl.semaphore_signal(barrier, inc=1, device_id={"dp": other}, device_id_type=MESH)
    pl.semaphore_wait(barrier, len(others))


def sigmoid(x):
    return 0.5 * jnp.tanh(0.5 * x) + 0.5


def norm_rows(wide):
    scale = lax.rsqrt(jnp.mean(wide * wide, -1, keepdims=True) + 1e-6)
    return (wide * scale).astype(BF16)


def forward_kernel(n, x_ref, wg_ref, wu_ref, wd_ref, g_ref, u_ref, d_ref, a_out, h_out, gate_out, up_out, hid_out,
                   own_g, own_u, own_d, h, a, at, hidden, wchunk, wdown, stage, hid, hid_t,
                   send, recv, own_sem, out_sem, w_sem, stage_sem, hid_sem, misc):
    me, chip, core, partner, right, left, far = places(n)
    layers = wg_ref.shape[0]
    tokens, d = x_ref.shape
    chunks, _, width = gate_out.shape[1:]
    chips = n // 2
    tile = stage.shape[2]
    tiles = tokens // tile
    span = g_ref.shape[2] // chips

    order = [(l, w, o) for l in range(layers) for w, o in ((g_ref, own_g), (u_ref, own_u), (d_ref, own_d))]

    loads = [pltpu.make_async_copy(src.at[l], o.at[l], own_sem.at[3 * l + i])
             for l in range(layers) for i, (src, o) in enumerate(((wg_ref, own_g), (wu_ref, own_u), (wd_ref, own_d)))]
    for one in loads:
        one.start()
    load_x = pltpu.make_async_copy(x_ref, h, misc.at[0])
    load_x.start()
    greet(partner, right, left)

    def rows(m, device, part=None):
        l, w, o = order[m]
        count = o.shape[1]
        if part is None:
            return w.at[l, pl.ds(device * count, count)]
        return w.at[l, pl.ds(device * count + part * (count // 2), count // 2)]

    def ag(m, kind):
        l, w, o = order[m]
        src, to = [
            (None, right), (None, left),
            (rows(m, left, 0), right), (rows(m, right, 1), left),
            (None, partner), (rows(m, left), partner), (rows(m, right), partner),
            (rows(m, far, 0), partner), (rows(m, far, 1), partner),
        ][kind]
        dst = rows(m, me) if src is None else src
        return pltpu.make_async_remote_copy(o.at[l] if src is None else src, dst, send.at[m, kind], recv.at[m, kind],
                                            device_id={"dp": to}, device_id_type=MESH)

    kept = []

    def begin(m):
        loads[m].wait()
        ag(m, 0).start()
        ag(m, 1).start()
        ag(m, 4).start()
        l, w, o = order[m]
        copy = pltpu.make_async_copy(o.at[l], rows(m, me), out_sem.at[m])
        copy.start()
        kept.append(copy)

    def pass_on(m):
        ag(m, 0).wait_recv()
        ag(m, 2).start()
        ag(m, 5).start()
        ag(m, 1).wait_recv()
        ag(m, 3).start()
        ag(m, 6).start()

    def hand_over(m):
        ag(m, 2).wait_recv()
        ag(m, 7).start()
        ag(m, 3).wait_recv()
        ag(m, 8).start()

    def complete(m):
        for kind in (4, 5, 6, 7, 8):
            ag(m, kind).wait_recv()
        kept[m].wait()

    begin(0)
    begin(1)
    load_x.wait()

    def norm_step(t, _):
        r = pl.ds(pl.multiple_of(t * 256, 256), 256)
        a[r, :] = norm_rows(h[r, :].astype(F32))
        return 0
    lax.fori_loop(0, tokens // 256, norm_step, 0)

    def turn(t, _):
        r = pl.ds(pl.multiple_of(t * 256, 256), 256)
        for c in range(chips):
            for part in range(2):
                at[pl.ds(part * (d // 2) + c * LANES, LANES), r] = a[r, pl.ds((2 * c + part) * LANES, LANES)].T
        return 0
    lax.fori_loop(0, tokens // 256, turn, 0)
    a_copy = pltpu.make_async_copy(at, a_out.at[0], misc.at[1])
    a_copy.start()

    def w_loads(l, j, slot):
        return [pltpu.make_async_copy(w.at[l, :, pl.ds(c * span + j * LANES, LANES)], wchunk.at[slot, i, :, pl.ds(c * LANES, LANES)],
                                      w_sem.at[slot, i, c])
                for i, w in enumerate((g_ref, u_ref)) for c in range(chips)]

    def gate_up(l, between, with_hidden):
        for one in w_loads(l, 0, 0):
            one.start()
        for j in range(chunks):
            slot = j % 2
            for one in w_loads(l, j, slot):
                one.wait()
            if j + 1 < chunks:
                for one in w_loads(l, j + 1, 1 - slot):
                    one.start()

            def step(t, _):
                half = lax.rem(t, 2)
                r = pl.ds(pl.multiple_of(t * tile, tile), tile)

                def outs(t_):
                    rr = pl.ds(pl.multiple_of(t_ * tile, tile), tile)
                    hh = lax.rem(t_, 2)
                    return [pltpu.make_async_copy(stage.at[hh, i], o.at[l, j, rr], stage_sem.at[hh, i])
                            for i, o in enumerate((gate_out, up_out))]

                @pl.when(t >= (2 if j == 0 else 0))
                def _():
                    for one in outs(t):
                        one.wait()
                for q in range(tile // 256):
                    rows_a = a[pl.ds(pl.multiple_of(t * tile + q * 256, 256), 256), :]
                    for i in range(2):
                        stage[half, i, pl.ds(q * 256, 256), :] = jnp.dot(rows_a, wchunk[slot, i], preferred_element_type=F32)
                    for e in range(256 // 32):
                        here = pl.ds(q * 256 + e * 32, 32)
                        gate, up = stage[half, 0, here, :], stage[half, 1, here, :]
                        sig = sigmoid(gate)
                        silu = gate * sig
                        value = (silu * up).astype(BF16)
                        hid[q, pl.ds(e * 32, 32), :] = value
                        if with_hidden:
                            hidden[pl.ds(pl.multiple_of(t * tile + q * 256 + e * 32, 32), 32), pl.ds(j * width, width)] = value
                        stage[half, 0, here, :] = silu
                        stage[half, 1, here, :] = up * (sig + silu * (1.0 - sig))
                    turned = hid[q].T
                    to = pl.ds(pl.multiple_of(t * tile + q * 256, 256), 256)
                    for c in range(chips):
                        for hh in range(2):
                            hid_t[slot, pl.ds(hh * (width // 2) + c * (LANES // 2), LANES // 2), to] = \
                                turned[c * LANES + hh * (LANES // 2):c * LANES + (hh + 1) * (LANES // 2), :]
                for one in outs(t):
                    one.start()
                return 0
            if j >= 2:
                pltpu.make_async_copy(hid_t.at[slot], hid_out.at[l, j], hid_sem.at[slot]).wait()
            lax.fori_loop(0, tiles, step, 0)
            pltpu.make_async_copy(hid_t.at[slot], hid_out.at[l, j], hid_sem.at[slot]).start()
            between(j)
        for slot in range(2):
            pltpu.make_async_copy(hid_t.at[slot], hid_out.at[l, 0], hid_sem.at[slot]).wait()
        for half in range(2):
            for i, o in enumerate((gate_out, up_out)):
                pltpu.make_async_copy(stage.at[half, i], o.at[l, 0, pl.ds(0, tile)], stage_sem.at[half, i]).wait()

    pass_on(0)
    pass_on(1)
    begin(2)
    begin(3)
    hand_over(0)
    hand_over(1)
    complete(0)
    complete(1)

    def first(j):
        if j == 2:
            pass_on(2)
            begin(4)
        if j == 4:
            pass_on(3)
    gate_up(0, first, True)

    hand_over(2)
    complete(2)
    down = [pltpu.make_async_copy(d_ref.at[0, pl.ds(c * span + j * LANES, LANES)], wdown.at[pl.ds(j * width + c * LANES, LANES)], misc.at[3 + j * chips + c])
            for j in range(chunks) for c in range(chips)]
    for one in down:
        one.start()
    a_copy.wait()
    for one in down:
        one.wait()

    def down_step(t, _):
        r = pl.ds(pl.multiple_of(t * tile, tile), tile)
        y = jnp.dot(hidden[r, :], wdown[...], preferred_element_type=F32).astype(BF16)
        h1 = (h[r, :].astype(F32) + y.astype(F32)).astype(BF16)
        h[r, :] = h1
        a[r, :] = norm_rows(h1.astype(F32))
        return 0
    lax.fori_loop(0, tiles, down_step, 0)
    h_copy = pltpu.make_async_copy(h, h_out, misc.at[2])
    h_copy.start()
    pass_on(4)
    begin(5)
    lax.fori_loop(0, tokens // 256, turn, 0)
    a_copy = pltpu.make_async_copy(at, a_out.at[1], misc.at[1])
    a_copy.start()
    hand_over(3)
    hand_over(4)
    complete(3)
    complete(4)

    def second(j):
        if j == 2:
            pass_on(5)
    gate_up(1, second, False)
    hand_over(5)
    complete(5)
    h_copy.wait()
    a_copy.wait()
    for m in range(len(order)):
        for kind in range(9):
            ag(m, kind).wait_send()


def forward(n, x, wg, wu, wd):
    tokens, d = x.shape
    layers, _, ff = wg.shape
    chips = n // 2
    width = chips * LANES
    chunks = ff // width
    tile = 512
    sds = jax.ShapeDtypeStruct
    dma = pltpu.SemaphoreType.DMA
    return pl.pallas_call(
        functools.partial(forward_kernel, n),
        name="forward",
        out_shape=(
            sds((layers, d, ff), BF16), sds((layers, d, ff), BF16), sds((layers, ff, d), BF16),
            sds((layers, d, tokens), BF16), sds((tokens, d), BF16),
            sds((layers, chunks, tokens, width), F32), sds((layers, chunks, tokens, width), F32),
            sds((layers, chunks, width, tokens), BF16),
        ),
        in_specs=[ANY] * 4,
        out_specs=(ANY,) * 8,
        scratch_shapes=[
            pltpu.VMEM(wg.shape, BF16), pltpu.VMEM(wu.shape, BF16), pltpu.VMEM(wd.shape, BF16),
            pltpu.VMEM((tokens, d), BF16), pltpu.VMEM((tokens, d), BF16), pltpu.VMEM((d, tokens), BF16), pltpu.VMEM((tokens, ff), BF16),
            pltpu.VMEM((2, 2, d, width), BF16), pltpu.VMEM((ff, d), BF16), pltpu.VMEM((2, 2, tile, width), F32),
            pltpu.VMEM((tile // 256, 256, width), BF16), pltpu.VMEM((2, width, tokens), BF16),
            dma((3 * layers, 9)), dma((3 * layers, 9)), dma((3 * layers,)), dma((3 * layers,)),
            dma((2, 2, chips)), dma((2, 2)), dma((2,)), dma((3 + chunks * chips,)),
        ],
        compiler_params=pltpu.CompilerParams(collective_id=0, has_side_effects=True, vmem_limit_bytes=60 * 1024 * 1024),
    )(x, wg, wu, wd)


SLOTS = 6
PAIR_SLOTS = 4
AHEAD = 4
PAIR_LAG, PASS_LAG, FINAL_LAG = 1, 3, 5


def backward_kernel(n, dy_ref, g_ref, u_ref, d_ref, a_ref, h_ref, gate_ref, up_ref, hid_ref, gg_out, gu_out, gd_out, sq_out,
                    ct, at, hs, da, hid_t, dg, du, dh, stage, wd, wgu, own, out_p, in_p, out_1, in_1, out_2, in_2, fin,
                    gg, gu, gd, sq, squares,
                    stage_sem, wd_sem, wgu_sem, h_sem, p_send, p_recv, s1_send, s1_recv, s2_send, s2_recv, f_send, f_recv, q_send, q_recv, misc):
    me, chip, core, partner, right, left, far = places(n)
    layers, chunks, tokens, width = gate_ref.shape
    d = dy_ref.shape[1]
    chips = n // 2
    span = g_ref.shape[2] // chips
    share = gd.shape[1]
    tile = stage.shape[2]
    tiles = tokens // tile
    sub = 256
    total = layers * chunks
    half = d // 2

    def layer_of(jj):
        return layers - 1 - jj // chunks

    def stage_loads(s):
        jj, t = s // tiles, lax.rem(s, tiles)
        slot = lax.rem(s, AHEAD)
        r = pl.ds(pl.multiple_of(t * tile, tile), tile)
        return [pltpu.make_async_copy(ref.at[layer_of(jj), lax.rem(jj, chunks), r], stage.at[slot, i], stage_sem.at[slot, i])
                for i, ref in enumerate((gate_ref, up_ref))]

    def wd_loads(jj):
        l, j, slot = layer_of(jj), lax.rem(jj, chunks), lax.rem(jj, 2)
        return [pltpu.make_async_copy(d_ref.at[l, pl.ds(pl.multiple_of(c * span + j * LANES, LANES), LANES)],
                                      wd.at[slot, pl.ds(c * LANES, LANES)], wd_sem.at[slot, c]) for c in range(chips)]

    def wgu_loads(jj):
        l, j, slot = layer_of(jj), lax.rem(jj, chunks), lax.rem(jj, 2)
        return [pltpu.make_async_copy(ref.at[l, :, pl.ds(pl.multiple_of(c * span + j * LANES, LANES), LANES)],
                                      wgu.at[slot, i, :, pl.ds(c * LANES, LANES)], wgu_sem.at[slot, i, c])
                for i, ref in enumerate((g_ref, u_ref)) for c in range(chips)]

    def at_load(l):
        return pltpu.make_async_copy(a_ref.at[l], at, misc.at[0])

    def h_load(t):
        slot = lax.rem(t, AHEAD)
        return pltpu.make_async_copy(h_ref.at[pl.ds(pl.multiple_of(t * sub, sub), sub)], hs.at[slot], h_sem.at[slot])

    def hid_load(jj):
        return pltpu.make_async_copy(hid_ref.at[layer_of(jj), lax.rem(jj, chunks)], hid_t, misc.at[2])

    first = [pltpu.make_async_copy(dy_ref, ct, misc.at[1])]
    for one in first + wd_loads(0) + stage_loads(0) + stage_loads(1):
        one.start()

    barrier = pltpu.get_barrier_semaphore()
    others = [lax.rem(me + k, n) for k in range(1, n)]
    for other in others:
        pl.semaphore_signal(barrier, inc=1, device_id={"dp": other}, device_id_type=MESH)

    def zero(t, _):
        da[pl.ds(pl.multiple_of(t * 128, 128), 128), :] = jnp.zeros((128, d), F32)
        return 0
    lax.fori_loop(0, tokens // 128, zero, 0)
    sq[...] = jnp.zeros_like(sq)
    pl.semaphore_wait(barrier, n - 1)
    for one in first:
        one.wait()
    for one in stage_loads(2) + stage_loads(3) + [hid_load(0)] + wgu_loads(0):
        one.start()
    at_load(layers - 1).start()
    for t in range(AHEAD):
        h_load(t).start()

    def remote(src, dst, ss, rs, to):
        return pltpu.make_async_remote_copy(src, dst, ss, rs, device_id={"dp": to}, device_id_type=MESH)

    def p_copy(k):
        o, s = lax.rem(k, 2), lax.rem(k, PAIR_SLOTS)
        return remote(out_p.at[o], in_p.at[s], p_send.at[o], p_recv.at[s], partner)

    def s1_copy(k, way):
        s = lax.rem(k, SLOTS)
        return remote(out_1.at[s, way], in_1.at[s, way], s1_send.at[s, way], s1_recv.at[s, way], (right, left)[way])

    def s2_copy(k, way):
        s = lax.rem(k, SLOTS)
        return remote(out_2.at[s, way], in_2.at[s, way], s2_send.at[s, way], s2_recv.at[s, way], (right, left)[way])

    mid = LANES // 2
    block_r, block_l, block_f = (lax.rem(chip + k, chips) for k in (1, chips - 1, 2))

    def pair_step(k):
        s, p = lax.rem(k, SLOTS), lax.rem(k, PAIR_SLOTS)
        p_copy(k).wait_recv()

        @pl.when(k >= SLOTS)
        def _():
            s1_copy(k - SLOTS, 0).wait_send()
            s1_copy(k - SLOTS, 1).wait_send()
        for way in range(2):
            rows = pl.ds(way * mid, mid)
            out_1[s, way] = (own[s, block_f, rows, :] + in_p[p, block_f, rows, :].astype(F32)).astype(BF16)
        s1_copy(k, 0).start()
        s1_copy(k, 1).start()
        for block in (block_r, block_l, chip):
            own[s, block] += in_p[p, block].astype(F32)

    def pass_step(k):
        s = lax.rem(k, SLOTS)
        s1_copy(k, 0).wait_recv()
        s1_copy(k, 1).wait_recv()

        @pl.when(k >= SLOTS)
        def _():
            s2_copy(k - SLOTS, 0).wait_send()
            s2_copy(k - SLOTS, 1).wait_send()
        for way, block in ((0, block_r), (1, block_l)):
            for part in range(2):
                rows = pl.ds(part * mid, mid)
                value = own[s, block, rows, :]
                if part == way:
                    value = value + in_1[s, way].astype(F32)
                out_2[s, way, rows, :] = value.astype(BF16)
        s2_copy(k, 0).start()
        s2_copy(k, 1).start()

    def f_copy(l, j, part):
        row = j * LANES + core * mid
        row = row - (row // share) * share
        rows = pl.ds(pl.multiple_of(row, mid), mid)
        return remote(fin.at[l, j, pl.ds(part * mid, mid)], gd.at[l, rows, pl.ds(part * width, width)],
                      f_send.at[l, j, part], f_recv.at[l, j, part], partner)

    def final_step(k, kind):
        s = lax.rem(k, SLOTS)
        jj = k // 3
        l, j = layer_of(jj), lax.rem(jj, chunks)
        s2_copy(k, 0).wait_recv()
        s2_copy(k, 1).wait_recv()
        value = own[s, chip] + in_2[s, 0].astype(F32) + in_2[s, 1].astype(F32)
        value = value.astype(BF16)
        wide = value.astype(F32)
        sq[...] += jnp.sum((wide * wide).reshape(LANES // 8, 8, width), 0)
        if kind:
            to = gg if kind == 1 else gu
            for c in range(chips):
                to[l, :, pl.ds(pl.multiple_of(c * span + j * LANES, LANES), LANES)] = value[:, c * LANES:(c + 1) * LANES]
        else:
            row = j * LANES + core * mid
            owner = row // share
            local = pl.multiple_of(row - owner * share, mid)

            @pl.when(owner == core)
            def _():
                for part in range(2):
                    gd[l, pl.ds(local, mid), pl.ds(part * width, width)] = value[part * mid:(part + 1) * mid, :]

            @pl.when(owner != core)
            def _():
                fin[l, j] = value
                f_copy(l, j, 0).start()
                f_copy(l, j, 1).start()

    def store(kind, ref, s, value):
        if kind:
            for c in range(chips):
                ref[s, c] = value[c * LANES:(c + 1) * LANES, :].astype(ref.dtype)
        else:
            for c in range(chips):
                for part in range(2):
                    ref[s, c, pl.ds(part * mid, mid), :] = value[c * mid:(c + 1) * mid, part * width:(part + 1) * width].astype(ref.dtype)

    def product(kind, which):
        if kind == 0:
            rows = pl.ds(pl.multiple_of(which * (width // 2), width // 2), width // 2)
            return jnp.dot(hid_t[rows, :], ct[...], preferred_element_type=F32)
        rows = pl.ds(pl.multiple_of(which * half, half), half)
        return jnp.dot(at[rows, :], (dg if kind == 1 else du)[...], preferred_element_type=F32)

    def tick(k, kind):
        def run(step, lag, *more):
            if lag > kind:
                pl.when(k >= lag)(lambda: step(k - lag, *more))
            else:
                step(k - lag, *more)

        @pl.when(k >= 2)
        def _():
            p_copy(k - 2).wait_send()
        store(kind, out_p, lax.rem(k, 2), product(kind, 1 - core))
        p_copy(k).start()
        run(pair_step, PAIR_LAG)
        run(pass_step, PASS_LAG)
        store(kind, own, lax.rem(k, SLOTS), product(kind, core))
        run(final_step, FINAL_LAG, (kind - FINAL_LAG) % 3)

    def chunk(jj, _):
        l, slot = layer_of(jj), lax.rem(jj, 2)

        @pl.when(jj == chunks)
        def _():
            at_load(0).start()

            def to_h(t, _):
                h_load(t).wait()
                for e in range(sub // 64):
                    here = pl.ds(pl.multiple_of(t * sub + e * 64, 64), 64)
                    wide = hs[lax.rem(t, AHEAD), pl.ds(e * 64, 64), :].astype(F32)
                    grad = da[here, :]
                    scale = lax.rsqrt(jnp.mean(wide * wide, -1, keepdims=True) + 1e-6)
                    back = grad * scale - wide * (scale * scale * scale * jnp.mean(grad * wide, -1, keepdims=True))
                    ct[here, :] = (ct[here, :].astype(F32) + back).astype(BF16)

                @pl.when(t + AHEAD < tokens // sub)
                def _():
                    h_load(t + AHEAD).start()
                return 0
            lax.fori_loop(0, tokens // sub, to_h, 0)

        for one in wd_loads(jj):
            one.wait()

        @pl.when(jj + 1 < total)
        def _():
            for one in wd_loads(jj + 1):
                one.start()

        @pl.when(jj + 1 < chunks)
        def _():
            for one in wgu_loads(jj + 1):
                one.start()

        def step(t, _):
            s = jj * tiles + t
            st = lax.rem(s, AHEAD)
            for one in stage_loads(s):
                one.wait()
            for q in range(tile // sub):
                r = pl.ds(pl.multiple_of(t * tile + q * sub, sub), sub)
                dh[q] = lax.dot_general(ct[r, :], wd[slot], NT, preferred_element_type=F32)
                for e in range(sub // 32):
                    here = pl.ds(q * sub + e * 32, 32)
                    there = pl.ds(pl.multiple_of(t * tile + q * sub + e * 32, 32), 32)
                    back = dh[q, pl.ds(e * 32, 32), :].astype(BF16).astype(F32)
                    du[there, :] = (back * stage[st, 0, here, :]).astype(BF16)
                    dg[there, :] = (back * stage[st, 1, here, :]).astype(BF16)

            @pl.when(s + AHEAD < total * tiles)
            def _():
                for one in stage_loads(s + AHEAD):
                    one.start()
            return 0
        lax.fori_loop(0, tiles, step, 0)

        @pl.when(lax.rem(jj, chunks) == 0)
        def _():
            at_load(layer_of(jj)).wait()

        def back(part):
            def back_step(t, _):
                r = pl.ds(pl.multiple_of(t * tile, tile), tile)
                da[r, :] += (lax.dot_general(dg[r, :], wgu[slot, 0], NT, preferred_element_type=F32)
                             + lax.dot_general(du[r, :], wgu[slot, 1], NT, preferred_element_type=F32))
                return 0

            @pl.when(jj < chunks)
            def _():
                lax.fori_loop(part * tiles // 2, (part + 1) * tiles // 2, back_step, 0)

        hid_load(jj).wait()
        tick(jj * 3, 0)

        @pl.when(jj + 1 < total)
        def _():
            hid_load(jj + 1).start()

        @pl.when(jj < chunks)
        def _():
            for one in wgu_loads(jj):
                one.wait()
        back(0)
        tick(jj * 3 + 1, 1)
        back(1)
        tick(jj * 3 + 2, 2)
        return 0
    lax.fori_loop(0, total, chunk, 0)

    last = 3 * total
    pair_step(last - 1)
    for k in range(last - PASS_LAG, last):
        pass_step(k)
        final_step(k - 2, (k - 2) % 3)
    final_step(last - 2, 1)
    final_step(last - 1, 2)

    squares[me] = jnp.sum(sq[...].reshape(8, width // LANES, LANES), 1)
    copies = [remote(squares.at[me], squares.at[me], q_send.at[k], q_recv.at[k], other) for k, other in enumerate(others)]
    for one in copies:
        one.start()
    outs = [pltpu.make_async_copy(a, b, misc.at[3 + i]) for i, (a, b) in enumerate(((gg, gg_out), (gu, gu_out)))]
    for one in outs:
        one.start()
    for l in range(layers):
        for j in range(chunks):
            row = j * LANES + core * mid

            @pl.when(row // share != core)
            def _():
                f_copy(l, j, 0).wait_send()
                f_copy(l, j, 1).wait_send()
            row = j * LANES + (1 - core) * mid

            @pl.when(row // share == core)
            def _():
                @pl.when(row // share != 1 - core)
                def _():
                    f_copy(l, j, 0).wait_recv()
                    f_copy(l, j, 1).wait_recv()
    outs.append(pltpu.make_async_copy(gd, gd_out, misc.at[5]))
    outs[-1].start()
    for one in copies:
        one.wait_recv()
    whole = squares[0]
    for k in range(1, n):
        whole = whole + squares[k]
    squares[n] = jnp.broadcast_to(jnp.sum(whole), (8, LANES))
    outs.append(pltpu.make_async_copy(squares.at[n], sq_out, misc.at[6]))
    outs[-1].start()
    for k in range(last - 2, last):
        p_copy(k).wait_send()
    for k in range(last - SLOTS, last):
        for way in range(2):
            s1_copy(k, way).wait_send()
            s2_copy(k, way).wait_send()
    for one in copies:
        one.wait_send()
    for one in outs:
        one.wait()


def backward(n, dy, g, u, dn, a, h, gate, up, hid):
    tokens, d = dy.shape
    layers, chunks, _, width = gate.shape
    ff = g.shape[2]
    chips = n // 2
    tile = 512
    sds = jax.ShapeDtypeStruct
    dma = pltpu.SemaphoreType.DMA
    v = pltpu.VMEM
    mid = LANES // 2
    grads = [((layers, d // n, ff), BF16), ((layers, d // n, ff), BF16), ((layers, ff // n, d), BF16)]
    return pl.pallas_call(
        functools.partial(backward_kernel, n),
        name="backward",
        out_shape=tuple(sds(*g_) for g_ in grads) + (sds((8, LANES), F32),),
        in_specs=[ANY] * 9,
        out_specs=(ANY,) * 4,
        scratch_shapes=[
            v((tokens, d), BF16), v((d, tokens), BF16), v((AHEAD, 256, d), BF16), v((tokens, d), F32),
            v((width, tokens), BF16), v((tokens, width), BF16), v((tokens, width), BF16),
            v((tile // 256, 256, width), F32), v((AHEAD, 2, tile, width), F32), v((2, width, d), BF16), v((2, 2, d, width), BF16),
            v((SLOTS, chips, LANES, width), F32), v((2, chips, LANES, width), BF16), v((PAIR_SLOTS, chips, LANES, width), BF16),
            v((SLOTS, 2, mid, width), BF16), v((SLOTS, 2, mid, width), BF16),
            v((SLOTS, 2, LANES, width), BF16), v((SLOTS, 2, LANES, width), BF16),
            v((layers, chunks, LANES, width), BF16),
            *(v(*g_) for g_ in grads), v((8, width), F32), v((n + 1, 8, LANES), F32),
            dma((AHEAD, 2)), dma((2, chips)), dma((2, 2, chips)), dma((AHEAD,)), dma((2,)), dma((PAIR_SLOTS,)),
            dma((SLOTS, 2)), dma((SLOTS, 2)), dma((SLOTS, 2)), dma((SLOTS, 2)),
            dma((layers, chunks, 2)), dma((layers, chunks, 2)), dma((n - 1,)), dma((n - 1,)), dma((7,)),
        ],
        compiler_params=pltpu.CompilerParams(collective_id=1, has_side_effects=True, vmem_limit_bytes=60 * 1024 * 1024),
    )(dy, g, u, dn, a, h, gate, up, hid)


def adamw(w, m, v, g):
    m = 0.9 * m + 0.1 * g
    v = 0.95 * v + 0.05 * g * g
    step = m * lax.rsqrt(v + 1e-8) + 0.1 * w
    return (w - 0.02 * step).astype(BF16), m, v


def update_kernel(count, squares_ref, *refs):
    factor = jnp.minimum(1.0, 0.5 * lax.rsqrt(squares_ref[0:1, 0:1] / count + 1e-30))
    for i in range(3):
        w, m, v, g = (refs[3 * which + i] for which in range(4))
        new = adamw(w[0].astype(F32), m[0], v[0], g[0].astype(F32) * factor)
        for which in range(3):
            refs[12 + 3 * which + i][0] = new[which]


def update(count, squares, weights, m, v, gradients):
    parts = 4
    specs = [pl.BlockSpec((1, w.shape[1] // parts, w.shape[2]), lambda l, r: (l, r, 0)) for w in weights]
    return pl.pallas_call(
        functools.partial(update_kernel, count),
        name="update",
        grid=(weights[0].shape[0], parts),
        out_shape=[jax.ShapeDtypeStruct(w.shape, dtype) for dtype in (BF16, F32, F32) for w in weights],
        in_specs=[pl.BlockSpec(squares.shape, lambda l, r: (0, 0))] + specs * 4,
        out_specs=specs * 3,
        compiler_params=pltpu.CompilerParams(vmem_limit_bytes=40_000 * 1024),
    )(squares, *weights, *m, *v, *gradients)


def solution(mesh):
    n = mesh.shape["dp"]

    def step(x, dy, *arrays):
        weights, m, v = (arrays[i : i + 3] for i in (0, 3, 6))
        g, u, dn, *saved = forward(n, x[0], *weights)
        *gradients, squares = backward(n, dy[0], g, u, dn, *saved)
        return tuple(update(n * sum(w.size for w in weights), squares, weights, m, v, gradients))

    states, cut = P(("rep", "dp"), None, None), P(None, "dp", None)
    return jax.shard_map(
        step,
        mesh=mesh,
        in_specs=(states, states) + (cut,) * 9,
        out_specs=(P("rep", "dp", None),) * 9,
        check_vma=False,
    )
```
